32 devices in a mesh: seq: 8 (over y, x, core), tensor: 4 (over z).
Axes of the slice: x: 2, y: 2, z: 4, core: 2. Of those that a mesh axis runs over, the one named last changes fastest.
Arguments:
- streams: float32 [4, 4096, 4096], P(None, 'seq', 'tensor'), may hold values from -8 to 8
- mix_weight: float32 [24, 4, 4096], P(None, None, 'tensor'), may hold values from -0.046875 to 0.046875
- mix_bias: float32 [24], replicated, may hold values from -4 to 4
- mix_scale: float32 [3], replicated, may hold values from 1 to 2
- norm_gain: bfloat16 [4096], replicated, may hold values from 0.25 to 1.75
- gate_weight: bfloat16 [4096, 7168], P('seq', 'tensor'), may hold values from -0.09375 to 0.09375
- up_weight: bfloat16 [4096, 7168], P('seq', 'tensor'), may hold values from -0.09375 to 0.09375
- down_weight: bfloat16 [7168, 4096], P('tensor', 'seq'), may hold values from -0.0625 to 0.0625
Outputs:
- new_streams: float32 [4, 4096, 4096], P(None, 'seq', 'tensor')
The draws below stay inside these ranges and needn't reach their ends.
All inputs are finite; a program needn't handle non-finite values.
Results may differ from the reference program's by a relative error of at most 0.01.
Values may be sent and summed in bfloat16 or wider, within the bound.
A program may use at most 128 MiB of HBM per device.

```python
import jax
import jax.numpy as jnp
from jax import lax

D = 4096
FF = 7168
STREAMS = 4
SWEEPS = 20
TOK_DEV = 512
TOKENS = 4096
LOGITS = 24
N_SEQ = 8
N_TENSOR = 4


def draw_streams(key, part):
    first = jax.random.fold_in(key, 11)
    second = jax.random.fold_in(key, 12)
    fifth = jax.random.fold_in(key, 15)
    groups = max(D // 64, 1)
    columns = D // groups
    scales = jnp.exp(jax.random.uniform(second, (STREAMS, TOKENS, groups, 1), jnp.float32, -1.2, 1.2))
    coarse = jnp.exp(jax.random.uniform(fifth, (STREAMS, TOKENS, 8, 1), jnp.float32, -1.5, 1.5))
    values = jax.random.normal(first, (STREAMS, TOKENS, groups, columns), jnp.float32) * scales
    values = values.reshape(STREAMS, TOKENS, 8, D // 8) * coarse
    return jnp.clip(values, -8.0, 8.0).reshape(STREAMS, TOKENS, D)


def steps_of(stream_key, dims, shards, least, high):
    level, own = 1.0, jax.random.fold_in(stream_key, 6)
    for dim, blocks in shards:
        steps = jnp.exp(jax.random.uniform(jax.random.fold_in(own, dim), (blocks,), jnp.float32, least / len(shards), high / len(shards)))
        level = level * jnp.repeat(steps, dims[dim] // blocks).reshape([-1 if axis == dim else 1 for axis in range(len(dims))])
    return level


def noise(own_key, shape, scale, bound, cuts=(), kind=jnp.bfloat16):
    array = scale * jax.random.normal(own_key, shape, jnp.float32)
    if cuts:
        array = array * steps_of(own_key, shape, cuts, -0.22, 0.18)
    return jnp.clip(array, -bound, bound).astype(kind)


def setup_inputs(seed: int = 0) -> dict:
    keys = jax.random.split(jax.random.key(seed), 9)
    return {
        "streams": draw_streams(jax.random.fold_in(keys[8], 71), 0),
        "mix_weight": noise(keys[1], (LOGITS, STREAMS, D), (STREAMS * D) ** -0.5, 0.046875, ((2, 4),), jnp.float32),
        "mix_bias": noise(keys[2], (LOGITS,), 1.0, 4.0, (), jnp.float32),
        "mix_scale": jnp.clip(jax.random.uniform(keys[3], (3,), jnp.float32, 1.0, 2.0), 1.0, 2.0),
        "norm_gain": jnp.clip(1.0 + 0.15 * jax.random.normal(keys[4], (D,), jnp.float32), 0.25, 1.75).astype(jnp.bfloat16),
        "gate_weight": noise(keys[5], (D, FF), D ** -0.5, 0.09375, ((0, 8), (1, 4))),
        "up_weight": noise(keys[6], (D, FF), D ** -0.5, 0.09375, ((0, 8), (1, 4))),
        "down_weight": noise(keys[7], (FF, D), FF ** -0.5, 0.0625, ((0, 4), (1, 8))),
    }


epsilon = 0.25

def coefficients(logits, mix_bias, mix_scale):
    pre_mix = jax.nn.sigmoid(mix_scale[0] * logits[:STREAMS] + mix_bias[:STREAMS, None])
    post_mix = 2.0 * jax.nn.sigmoid(mix_scale[1] * logits[STREAMS:2 * STREAMS] + mix_bias[STREAMS:2 * STREAMS, None])
    start_mix = jnp.exp(mix_scale[2] * logits[2 * STREAMS:] + mix_bias[2 * STREAMS:, None])
    start_mix = start_mix.reshape(STREAMS, STREAMS, logits.shape[1])

    def balance(iteration, matrix):
        matrix = matrix / lax.optimization_barrier(jnp.sum(matrix, axis=1, keepdims=True))
        return matrix / lax.optimization_barrier(jnp.sum(matrix, axis=0, keepdims=True))
    return (pre_mix, post_mix, lax.fori_loop(0, SWEEPS, balance, start_mix))

def layer_block(block, streams, mix_weight, mix_bias, mix_scale, norm_gain, gate_weight, up_weight, down_weight):
    current = lax.dynamic_slice_in_dim(streams, (block * TOK_DEV).astype(jnp.int32), TOK_DEV, 1)
    squares = lax.optimization_barrier(jnp.sum(current * current, axis=(0, 2)))
    inverse = lax.rsqrt(squares / (STREAMS * D) + epsilon)
    raw_logits = jnp.einsum('lkd,ktd->lt', mix_weight, current, precision=lax.Precision.HIGHEST)
    pre_mix, post_mix, res_mix = coefficients(raw_logits * inverse[None, :], mix_bias, mix_scale)
    layer_in = lax.optimization_barrier(jnp.sum(pre_mix[:, :, None] * current, axis=0)).astype(jnp.bfloat16)
    as_float = layer_in.astype(jnp.float32)
    mean_square = lax.optimization_barrier(jnp.mean(as_float * as_float, axis=1, keepdims=True))
    normed = (as_float * lax.rsqrt(mean_square + epsilon) * norm_gain.astype(jnp.float32)).astype(jnp.bfloat16)
    gate_value = jnp.dot(normed, gate_weight, preferred_element_type=jnp.float32)
    up_value = jnp.dot(normed, up_weight, preferred_element_type=jnp.float32)
    hidden = (jax.nn.silu(gate_value) * up_value).astype(jnp.bfloat16)
    share = FF // N_TENSOR
    layer_out = jnp.zeros((TOK_DEV, D), jnp.float32)
    for group in range(N_TENSOR):
        partial_out = jnp.dot(hidden[:, group * share:(group + 1) * share], down_weight[group * share:(group + 1) * share], preferred_element_type=jnp.float32)
        rounded = lax.optimization_barrier(partial_out.astype(jnp.bfloat16))
        layer_out = layer_out + rounded.astype(jnp.float32)
    outputs = []
    for target in range(STREAMS):
        mixed = post_mix[target][:, None] * layer_out
        for source in range(STREAMS):
            mixed = mixed + res_mix[target, source][:, None] * current[source]
        outputs.append(mixed)
    return jnp.stack(outputs)

def reference(streams, mix_weight, mix_bias, mix_scale, norm_gain, gate_weight, up_weight, down_weight):

    def one_block(block):
        return layer_block(block, streams, mix_weight, mix_bias, mix_scale, norm_gain, gate_weight, up_weight, down_weight)
    blocks = lax.map(one_block, jnp.arange(N_SEQ, dtype=jnp.int32))
    return jnp.moveaxis(blocks, 0, 1).reshape(STREAMS, TOKENS, D)
```

```python
import functools

import jax
import jax.numpy as jnp
from jax import lax
from jax.experimental import pallas as pl
from jax.experimental.pallas import tpu as pltpu
from jax.sharding import PartitionSpec as P

STREAMS = 4
SWEEPS = 20
EPSILON = 0.25
LANES = 128
MESH = pl.DeviceIdType.MESH
HIGHEST = lax.Precision.HIGHEST


def flip(index, offset):
    bit, out = 1, index
    while bit <= offset:
        if offset & bit:
            out = out + bit - 2 * bit * lax.rem(lax.div(index, bit), 2)
        bit *= 2
    return out


def last_bit(offset, order):
    if offset & 1:
        return 1
    return [b for b in order if offset & b][-1]


def width_of(size, limit):
    width = limit
    while size % width:
        width -= LANES
    return width


def block_kernel(
    n_seq,
    n_tensor,
    bias_ref,
    scale_ref,
    mix_ref,
    gain_ref,
    streams_ref,
    gate_ref,
    up_ref,
    down_ref,
    out_ref,
    coef_ref,
    gate_buf,
    up_buf,
    down_buf,
    blocks,
    normed,
    hidden,
    arrived,
    tiles,
    stats,
    columns,
    tile_sem,
    weight_send,
    weight_recv,
    down_send,
    down_recv,
    stat_send,
    stat_recv,
    input_send,
    input_recv,
    part_send,
    part_recv,
):
    s, z = lax.axis_index("seq"), lax.axis_index("tensor")
    tokens, width = out_ref.shape
    features = width * n_tensor
    rows = features // n_seq
    n_gate, _, gate_width = gate_buf.shape
    n_down, pairs, units, block_width = down_buf.shape
    half = block_width // 2
    per = n_seq // n_tensor
    pair_blocks = per // 2
    own_blocks = n_down * pair_blocks
    piece = tiles.shape[2]
    tile = 2 * piece
    n_tiles = tokens // tile

    bits = []
    bit = 2
    while bit < n_seq:
        bits.append(bit)
        bit *= 2
    orders = (bits, bits[::-1])
    everything = n_seq - 2
    even = sorted(range(2, n_seq, 2), key=lambda o: (bin(o).count("1"), o))

    def peer(offset):
        return (flip(s, offset), z)

    def across(shift):
        return (s, lax.rem(z + shift, n_tensor))

    barrier = pltpu.get_barrier_semaphore()
    for b in [1] + bits:
        pl.semaphore_signal(barrier, inc=1, device_id=peer(b), device_id_type=MESH)
    for shift in range(1, n_tensor):
        pl.semaphore_signal(barrier, inc=1, device_id=across(shift), device_id_type=MESH)
    pl.semaphore_wait(barrier, len(bits) + n_tensor)

    weights = ((gate_ref, gate_buf), (up_ref, up_buf))

    def gate_slot(kind, c, o):
        return weights[kind][1].at[c, pl.ds(o * rows, rows), :]

    def gate_own(kind, c):
        return weights[kind][0].at[:, pl.ds(pl.multiple_of(c * gate_width, LANES), gate_width)]

    def gate_copy(kind, c, o):
        b = last_bit(o, orders[kind])
        source = gate_own(kind, c) if o == b else gate_slot(kind, c, o ^ b)
        return pltpu.make_async_remote_copy(
            src_ref=source,
            dst_ref=gate_slot(kind, c, o),
            send_sem=weight_send.at[kind, c, o],
            recv_sem=weight_recv.at[kind, c, o],
            device_id=peer(b),
            device_id_type=MESH,
        )

    def gate_local(kind, c):
        return pltpu.make_async_copy(gate_own(kind, c), gate_slot(kind, c, 0), weight_recv.at[kind, c, 0])

    def down_slot(c, o):
        return down_buf.at[c, o // 2, :, pl.ds((o % 2) * half, half)]

    def down_own(c):
        return down_ref.at[:, pl.ds(c * half, half)]

    def down_copy(c, o):
        b = last_bit(o, orders[c % 2])
        return pltpu.make_async_remote_copy(
            src_ref=down_own(c) if o == b else down_slot(c, o ^ b),
            dst_ref=down_slot(c, o),
            send_sem=down_send.at[c, o],
            recv_sem=down_recv.at[c, o],
            device_id=peer(b),
            device_id_type=MESH,
        )

    def down_local(c):
        return pltpu.make_async_copy(down_own(c), down_slot(c, 0), down_recv.at[c, 0])

    def children(o, order):
        return [t for t in range(1, n_seq) if t ^ last_bit(t, order) == o and t != o]

    @pl.loop(0, n_gate)
    def _(c):
        for kind in (0, 1):
            for o in sorted(children(0, orders[kind]), key=lambda t: -t):
                gate_copy(kind, c, o).start()
            gate_local(kind, c).start()

    def tile_copy(i, slot):
        at = pl.ds(pl.multiple_of(i * tile + slot * piece, piece), piece)
        return pltpu.make_async_copy(streams_ref.at[:, at, :], tiles.at[slot], tile_sem.at[slot])

    def fetch(i, slot):
        @pl.when(i < n_tiles)
        def _():
            tile_copy(i, slot).start()

    for slot in (0, 1):
        tile_copy(0, slot).start()

    @pl.loop(0, n_tiles)
    def _(i):
        contract = (((1,), (1,)), ((), ()))
        found = []
        for slot in (0, 1):
            tile_copy(i, slot).wait()
            logits = square = 0.0
            for k in range(STREAMS):
                current = tiles[slot, k]
                logits += lax.dot_general(
                    mix_ref[:, k, :], current, contract, precision=HIGHEST, preferred_element_type=jnp.float32
                )
                square += current * current
            squares = lax.dot_general(
                jnp.ones((8, width), jnp.float32),
                square,
                contract,
                precision=HIGHEST,
                preferred_element_type=jnp.float32,
            )
            found.append(jnp.concatenate([logits, squares]))
            fetch(i + 1, slot)
        stats[0, :, pl.ds(pl.multiple_of(i * tile, LANES), tile)] = jnp.concatenate(found, axis=1)

    def stat_copy(shift):
        return pltpu.make_async_remote_copy(
            src_ref=stats.at[0],
            dst_ref=stats.at[shift],
            send_sem=stat_send.at[shift],
            recv_sem=stat_recv.at[shift],
            device_id=across(shift),
            device_id_type=MESH,
        )

    for shift in range(1, n_tensor):
        stat_copy(shift).start()
    for slot in (0, 1):
        tile_copy(0, slot).start()
    for shift in range(1, n_tensor):
        stat_copy(shift).wait_recv()
    total = stats[0]
    for shift in range(1, n_tensor):
        total = total + stats[shift]
    n_logits = mix_ref.shape[0]
    logits = total[:n_logits] * lax.rsqrt(total[n_logits : n_logits + 1] / (STREAMS * features) + EPSILON)

    def scaled(which, at):
        return scale_ref[which] * logits[at : at + 1] + bias_ref[at]

    pre = [jax.nn.sigmoid(scaled(0, k)) for k in range(STREAMS)]
    columns[...] = jnp.concatenate(pre + [jnp.zeros((LANES - STREAMS, tokens), jnp.float32)]).T

    def input_copy(i, shift):
        at = (pl.ds(z * own_blocks, own_blocks), pl.ds(pl.multiple_of(i * tile, tile), tile), slice(None))
        return pltpu.make_async_remote_copy(
            src_ref=blocks.at[at],
            dst_ref=blocks.at[at],
            send_sem=input_send.at[shift, i],
            recv_sem=input_recv.at[shift, i],
            device_id=across(shift),
            device_id_type=MESH,
        )

    @pl.loop(0, n_tiles)
    def _(i):
        for slot in (0, 1):
            tile_copy(i, slot).wait()
            at = pl.ds(pl.multiple_of(i * tile + slot * piece, piece), piece)
            weight = columns[at, :]
            mixed = 0.0
            for k in range(STREAMS):
                mixed += weight[:, k : k + 1] * tiles[slot, k]
            mixed = mixed.astype(jnp.bfloat16)
            for j in range(own_blocks):
                blocks[z * own_blocks + j, at, :] = mixed[:, j * block_width : (j + 1) * block_width]
            fetch(i + 1, slot)
        for shift in range(1, n_tensor):
            input_copy(i, shift).start()

    post = [2.0 * jax.nn.sigmoid(scaled(1, STREAMS + k)) for k in range(STREAMS)]
    start = tuple(jnp.exp(scaled(2, 2 * STREAMS + k)) for k in range(STREAMS * STREAMS))

    def balance(_, matrix):
        grid = [list(matrix[k * STREAMS : (k + 1) * STREAMS]) for k in range(STREAMS)]
        for k in range(STREAMS):
            row = grid[k][0] + grid[k][1] + grid[k][2] + grid[k][3]
            grid[k] = [g / row for g in grid[k]]
        for j in range(STREAMS):
            column = grid[0][j] + grid[1][j] + grid[2][j] + grid[3][j]
            for k in range(STREAMS):
                grid[k][j] = grid[k][j] / column
        return tuple(g for line in grid for g in line)

    res = lax.fori_loop(0, SWEEPS, balance, start)
    filler = LANES - STREAMS - STREAMS * STREAMS
    coef_ref[...] = jnp.concatenate(post + list(res) + [jnp.zeros((filler, tokens), jnp.float32)]).T

    @pl.loop(0, n_gate)
    def _(c):
        for o in even:
            if o == everything:
                continue
            for kind in (0, 1):
                gate_copy(kind, c, o).wait_recv()
                for t in children(o, orders[kind]):
                    gate_copy(kind, c, t).start()

    for c in range(n_down):
        for o in sorted(children(0, orders[c % 2]), key=lambda t: -t):
            down_copy(c, o).start()
        down_local(c).start()

    granule = min(rows, block_width)

    @pl.loop(0, n_tiles)
    def _(i):
        at = pl.ds(pl.multiple_of(i * tile, tile), tile)
        for shift in range(1, n_tensor):
            input_copy(i, shift).wait_recv()
        square = 0.0
        for j in range(n_tensor * own_blocks):
            value = blocks[j, at, :].astype(jnp.float32)
            square += value * value
        inverse = lax.rsqrt(jnp.sum(square, axis=1, keepdims=True) / features + EPSILON)
        for src in range(n_seq):
            o = flip(s, src)
            for g in range(rows // granule):
                col = src * rows + g * granule
                part = pl.ds(col % block_width, granule)
                value = blocks[col // block_width, at, part].astype(jnp.float32)
                value = value * inverse * gain_ref[:, pl.ds(col, granule)].astype(jnp.float32)
                to = pl.ds(pl.multiple_of(o * rows + g * granule, LANES), granule)
                normed[at, to] = value.astype(jnp.bfloat16)

    @pl.loop(0, n_gate)
    def _(c):
        for kind in (0, 1):
            gate_copy(kind, c, everything).wait_recv()
            gate_copy(kind, c, everything + 1).start()
        for kind in (0, 1):
            gate_local(kind, c).wait()
            for o in range(1, n_seq, 2):
                gate_copy(kind, c, o).wait_recv()
        gate_value = jnp.dot(normed[...], gate_buf[c], preferred_element_type=jnp.float32)
        up_value = jnp.dot(normed[...], up_buf[c], preferred_element_type=jnp.float32)
        to = pl.ds(pl.multiple_of(c * gate_width, LANES), gate_width)
        hidden[:, to] = (gate_value / (1.0 + jnp.exp(-gate_value)) * up_value).astype(jnp.bfloat16)

    for shift in range(1, n_tensor):

        @pl.loop(0, n_tiles)
        def _(i):
            input_copy(i, shift).wait_send()

    def part_copy(c, q, shift):
        source = flip(s, 2 * q)
        to = lax.div(source, per)
        at = c * pair_blocks + lax.rem(lax.div(source, 2), pair_blocks)
        return pltpu.make_async_remote_copy(
            src_ref=blocks.at[to * own_blocks + at],
            dst_ref=arrived.at[shift - 1, at],
            send_sem=part_send.at[c, q],
            recv_sem=part_recv.at[shift - 1, at],
            device_id=(s, to),
            device_id_type=MESH,
        )

    def part_arrival(shift, at):
        return pltpu.make_async_remote_copy(
            src_ref=blocks.at[at],
            dst_ref=arrived.at[shift - 1, at],
            send_sem=part_send.at[0, 0],
            recv_sem=part_recv.at[shift - 1, at],
            device_id=across(shift),
            device_id_type=MESH,
        )

    def project(c, q):
        value = jnp.dot(hidden[...], down_buf[c, q], preferred_element_type=jnp.float32).astype(jnp.bfloat16)
        source = flip(s, 2 * q)
        to = lax.div(source, per)
        at = to * own_blocks + c * pair_blocks + lax.rem(lax.div(source, 2), pair_blocks)
        core = lax.rem(s, 2)
        blocks[at, :, pl.ds(pl.multiple_of(core * half, LANES), half)] = value[:, :half]
        blocks[at, :, pl.ds(pl.multiple_of((1 - core) * half, LANES), half)] = value[:, half:]
        for shift in range(1, n_tensor):

            @pl.when(lax.rem(z + shift, n_tensor) == to)
            def _():
                part_copy(c, q, shift).start()

    for c in range(n_down):
        down_local(c).wait()
        down_copy(c, 1).wait_recv()
        project(c, 0)
    for c in range(n_down):
        for o in even:
            if o == everything:
                continue
            down_copy(c, o).wait_recv()
            for t in children(o, orders[c % 2]):
                down_copy(c, t).start()
        for o in even:
            if o != everything:
                down_copy(c, o + 1).wait_recv()
                project(c, o // 2)
    for c in range(n_down):
        down_copy(c, everything).wait_recv()
        down_copy(c, everything + 1).start()
        down_copy(c, everything + 1).wait_recv()
        project(c, everything // 2)

    for at in range(own_blocks):
        c, p = at // pair_blocks, at % pair_blocks
        for shift in range(1, n_tensor):
            part_arrival(shift, at).wait_recv()
        for h in (0, 1):
            part = pl.ds(h * half, half)
            value = blocks[z * own_blocks + at, :, part].astype(jnp.float32)
            for shift in range(1, n_tensor):
                value += arrived[shift - 1, at, :, part].astype(jnp.float32)
            out_ref[:, pl.ds((2 * p + h) * rows + c * half, half)] = value

    for shift in range(1, n_tensor):
        stat_copy(shift).wait_send()

    @pl.loop(0, n_gate)
    def _(c):
        for kind in (0, 1):
            for o in range(1, n_seq):
                gate_copy(kind, c, o).wait_send()

    for c in range(n_down):
        for o in range(1, n_seq):
            down_copy(c, o).wait_send()
        for q in range(pairs):
            to = lax.div(flip(s, 2 * q), per)

            @pl.when(to != z)
            def _():
                part_copy(c, q, 1).wait_send()


def feed_forward(mesh, streams, mix_weight, mix_bias, mix_scale, norm_gain, gate_weight, up_weight, down_weight):
    n_seq, n_tensor = mesh.shape["seq"], mesh.shape["tensor"]
    tokens, width = streams.shape[1:]
    units = gate_weight.shape[1]
    rows = gate_weight.shape[0]
    features = width * n_tensor
    gate_width = width_of(units, 2 * LANES)
    n_gate = units // gate_width
    half = LANES
    n_down = down_weight.shape[1] // half
    own_blocks = width // (2 * half)
    tile = LANES
    n_tiles = tokens // tile
    hbm, vmem = pl.BlockSpec(memory_space=pl.ANY), pl.BlockSpec(memory_space=pltpu.VMEM)
    smem = pl.BlockSpec(memory_space=pltpu.SMEM)
    dma = pltpu.SemaphoreType.DMA
    return pl.pallas_call(
        functools.partial(block_kernel, n_seq, n_tensor),
        out_shape=(
            jax.ShapeDtypeStruct((tokens, width), jnp.float32),
            jax.ShapeDtypeStruct((tokens, LANES), jnp.float32),
        ),
        in_specs=[smem, smem, vmem, vmem, hbm, hbm, hbm, hbm],
        out_specs=(vmem, vmem),
        scratch_shapes=[
            pltpu.VMEM((n_gate, n_seq * rows, gate_width), jnp.bfloat16),
            pltpu.VMEM((n_gate, n_seq * rows, gate_width), jnp.bfloat16),
            pltpu.VMEM((n_down, n_seq // 2, units, 2 * half), jnp.bfloat16),
            pltpu.VMEM((n_tensor * own_blocks, tokens, 2 * half), jnp.bfloat16),
            pltpu.VMEM((tokens, features), jnp.bfloat16),
            pltpu.VMEM((tokens, units), jnp.bfloat16),
            pltpu.VMEM((n_tensor - 1, own_blocks, tokens, 2 * half), jnp.bfloat16),
            pltpu.VMEM((2, STREAMS, tile // 2, width), jnp.float32),
            pltpu.VMEM((n_tensor, mix_weight.shape[0] + 8, tokens), jnp.float32),
            pltpu.VMEM((tokens, LANES), jnp.float32),
            dma((2,)),
            dma((2, n_gate, n_seq)),
            dma((2, n_gate, n_seq)),
            dma((n_down, n_seq)),
            dma((n_down, n_seq)),
            dma((n_tensor,)),
            dma((n_tensor,)),
            dma((n_tensor, n_tiles)),
            dma((n_tensor, n_tiles)),
            dma((n_down, n_seq // 2)),
            dma((n_tensor - 1, own_blocks)),
        ],
        compiler_params=pltpu.CompilerParams(
            collective_id=0, has_side_effects=True, vmem_limit_bytes=67_043_328
        ),
    )(mix_bias, mix_scale, mix_weight, norm_gain.reshape(1, -1), streams, gate_weight, up_weight, down_weight)


def mix_kernel(streams_ref, layer_ref, mix_ref, out_ref):
    layer_out = layer_ref[...]
    for target in range(STREAMS):
        mixed = mix_ref[:, target : target + 1] * layer_out
        for source in range(STREAMS):
            at = STREAMS * (1 + target) + source
            mixed = mixed + mix_ref[:, at : at + 1] * streams_ref[source]
        out_ref[target] = mixed


def mix_streams(streams, layer_out, mixes):
    tokens, width = layer_out.shape
    tile = 64
    return pl.pallas_call(
        mix_kernel,
        grid=(tokens // tile,),
        in_specs=[
            pl.BlockSpec((STREAMS, tile, width), lambda i: (0, i, 0)),
            pl.BlockSpec((tile, width), lambda i: (i, 0)),
            pl.BlockSpec((tile, mixes.shape[1]), lambda i: (i, 0)),
        ],
        out_specs=pl.BlockSpec((STREAMS, tile, width), lambda i: (0, i, 0)),
        out_shape=jax.ShapeDtypeStruct(streams.shape, jnp.float32),
        compiler_params=pltpu.CompilerParams(vmem_limit_bytes=16 * 1024 * 1024),
    )(streams, layer_out, mixes)


def solution(mesh):
    def body(streams, *rest):
        layer_out, mixes = feed_forward(mesh, streams, *rest)
        return mix_streams(streams, layer_out, mixes)

    placed = (
        P(None, "seq", "tensor"),
        P(None, None, "tensor"),
        P(),
        P(),
        P(),
        P("seq", "tensor"),
        P("seq", "tensor"),
        P("tensor", "seq"),
    )
    return jax.shard_map(body, mesh=mesh, in_specs=placed, out_specs=P(None, "seq", "tensor"), check_vma=False)
```

```python
import functools
import math

import jax
import jax.numpy as jnp
from jax import lax
from jax.experimental import pallas as pl
from jax.experimental.pallas import tpu as pltpu
from jax.sharding import PartitionSpec as P

STREAMS = 4
SWEEPS = 20
EPSILON = 0.25
LANES = 128
SUBLANES = 8
SPLITS = 2
MIX_TILES = 8
MESH = pl.DeviceIdType.MESH
HIGHEST = lax.Precision.HIGHEST


def flip(index, offset):
    bit, out = 1, index
    while bit <= offset:
        if offset & bit:
            out = out + bit - 2 * bit * lax.rem(lax.div(index, bit), 2)
        bit *= 2
    return out


def last_bit(offset, order):
    if offset & 1:
        return 1
    return [b for b in order if offset & b][-1]


def width_of(size, limit):
    width = limit
    while size % width:
        width -= LANES
    return width


def block_kernel(
    n_seq,
    n_tensor,
    bias_ref,
    scale_ref,
    mix_ref,
    gain_ref,
    streams_ref,
    gate_ref,
    up_ref,
    down_ref,
    out_ref,
    coef_ref,
    gate_buf,
    up_buf,
    down_buf,
    blocks,
    normed,
    hidden,
    arrived,
    tiles,
    mix_parts,
    stats,
    columns,
    tile_sem,
    weight_send,
    weight_local,
    weight_recv,
    weight_pair,
    down_send,
    down_local,
    down_recv,
    down_pair,
    stat_send,
    stat_recv,
    input_send,
    input_recv,
    part_send,
    part_recv,
    free,
):
    s, z = lax.axis_index("seq"), lax.axis_index("tensor")
    tokens, width = out_ref.shape
    features = width * n_tensor
    rows = features // n_seq
    n_gate, _, gate_width = gate_buf.shape
    n_down, pairs, units, block_width = down_buf.shape
    half = block_width // 2
    per = n_seq // n_tensor
    pair_blocks = per // 2
    own_blocks = n_down * pair_blocks
    piece = tiles.shape[2]
    tile = 2 * piece
    n_tiles = tokens // tile

    bits = []
    bit = 2
    while bit < n_seq:
        bits.append(bit)
        bit *= 2
    orders = (bits, bits[::-1])
    everything = n_seq - 2
    last = len(bits)

    def stage(o):
        return bin(o - o % 2).count("1")

    stages = [[o for o in range(0, n_seq, 2) if stage(o) == r] for r in range(last + 1)]

    def await_bytes(ref, sem):
        pltpu.make_async_copy(ref, ref, sem).wait()

    def peer(offset):
        return (flip(s, offset), z)

    def across(shift):
        return (s, lax.rem(z + shift, n_tensor))

    barrier = pltpu.get_barrier_semaphore()
    for b in [1] + bits:
        pl.semaphore_signal(barrier, inc=1, device_id=peer(b), device_id_type=MESH)
    for shift in range(1, n_tensor):
        pl.semaphore_signal(barrier, inc=1, device_id=across(shift), device_id_type=MESH)
    pl.semaphore_wait(barrier, len(bits) + n_tensor)

    weights = ((gate_ref, gate_buf), (up_ref, up_buf))

    def gate_slot(kind, c, o):
        return weights[kind][1].at[c, pl.ds(o * rows, rows), :]

    def gate_own(kind, c):
        return weights[kind][0].at[:, pl.ds(pl.multiple_of(c * gate_width, LANES), gate_width)]

    def gate_copy(kind, c, o):
        b = last_bit(o, orders[kind])
        source = gate_own(kind, c) if o == b else gate_slot(kind, c, o ^ b)
        return pltpu.make_async_remote_copy(
            src_ref=source,
            dst_ref=gate_slot(kind, c, o),
            send_sem=weight_send.at[kind],
            recv_sem=weight_pair.at[c] if o % 2 else weight_recv.at[c, stage(o) - 1],
            device_id=peer(b),
            device_id_type=MESH,
        )

    def gate_copy_local(kind, c):
        return pltpu.make_async_copy(gate_own(kind, c), gate_slot(kind, c, 0), weight_local.at[kind])

    def gate_arrival(c, r):
        await_bytes(gate_buf.at[c, pl.ds(0, 2 * len(stages[r]) * rows), :], weight_recv.at[c, r - 1])

    depth = units // 2

    def down_slot(kind, c, o):
        return down_buf.at[c, o // 2, pl.ds(kind * depth, depth), pl.ds((o % 2) * half, half)]

    def down_own(kind, c):
        return down_ref.at[pl.ds(kind * depth, depth), pl.ds(pl.multiple_of(c * half, LANES), half)]

    def down_copy(kind, c, o):
        b = last_bit(o, orders[kind])
        return pltpu.make_async_remote_copy(
            src_ref=down_own(kind, c) if o == b else down_slot(kind, c, o ^ b),
            dst_ref=down_slot(kind, c, o),
            send_sem=down_send.at[o % 2],
            recv_sem=down_pair.at[c, stage(o)] if o % 2 else down_recv.at[c, stage(o) - 1],
            device_id=peer(b),
            device_id_type=MESH,
        )

    def down_copy_local(kind, c):
        return pltpu.make_async_copy(down_own(kind, c), down_slot(kind, c, 0), down_local.at[0])

    def down_share(c, r):
        return down_buf.at[c, pl.ds(0, len(stages[r])), :, pl.ds(0, half)]

    def down_arrival(c, r):
        await_bytes(down_share(c, r), down_recv.at[c, r - 1])

    def down_pair_arrival(c, r):
        await_bytes(down_share(c, r), down_pair.at[c, r])

    def children(o, order):
        return [t for t in range(1, n_seq) if t ^ last_bit(t, order) == o and t != o]

    @pl.loop(0, n_gate)
    def _(c):
        for kind in (0, 1):
            for o in sorted(children(0, orders[kind]), key=lambda t: -t):
                gate_copy(kind, c, o).start()
            gate_copy_local(kind, c).start()

    def tile_copy(i, slot):
        at = pl.ds(pl.multiple_of(i * tile + slot * piece, piece), piece)
        return pltpu.make_async_copy(streams_ref.at[:, at, :], tiles.at[slot], tile_sem.at[slot])

    def fetch(i, slot):
        @pl.when(i < n_tiles)
        def _():
            tile_copy(i, slot).start()

    for slot in (0, 1):
        tile_copy(0, slot).start()

    def halves(value):
        high = value.astype(jnp.bfloat16)
        return high, (value - high.astype(jnp.float32)).astype(jnp.bfloat16)

    n_logits = mix_ref.shape[0]
    for k in range(STREAMS):
        mix_parts[k] = jnp.concatenate(halves(mix_ref[:, k, :]))

    @pl.loop(0, n_tiles)
    def _(i):
        contract = (((1,), (1,)), ((), ()))
        found = []
        for slot in (0, 1):
            tile_copy(i, slot).wait()
            product = square = 0.0
            for k in range(STREAMS):
                current = tiles[slot, k]
                product += lax.dot_general(
                    mix_parts[k], jnp.concatenate(halves(current)), contract, preferred_element_type=jnp.float32
                )
                square += current * current
            product = product[:n_logits] + product[n_logits:]
            logits = product[:, :piece] + product[:, piece:]
            square = sum(square[:, j : j + LANES] for j in range(0, width, LANES))
            squares = lax.dot_general(
                jnp.ones((8, LANES), jnp.float32),
                square,
                contract,
                precision=HIGHEST,
                preferred_element_type=jnp.float32,
            )
            found.append(jnp.concatenate([logits, squares]))
            fetch(i + 1, slot)
        stats[0, :, pl.ds(pl.multiple_of(i * tile, LANES), tile)] = jnp.concatenate(found, axis=1)

    def stat_copy(shift):
        return pltpu.make_async_remote_copy(
            src_ref=stats.at[0],
            dst_ref=stats.at[shift],
            send_sem=stat_send.at[0],
            recv_sem=stat_recv.at[0],
            device_id=across(shift),
            device_id_type=MESH,
        )

    for shift in range(1, n_tensor):
        stat_copy(shift).start()
    for slot in (0, 1):
        tile_copy(0, slot).start()
    await_bytes(stats.at[pl.ds(1, n_tensor - 1)], stat_recv.at[0])
    total = stats[0]
    for shift in range(1, n_tensor):
        total = total + stats[shift]
    logits = total[:n_logits] * lax.rsqrt(total[n_logits : n_logits + 1] / (STREAMS * features) + EPSILON)

    def scaled(which, at):
        return scale_ref[which] * logits[at : at + 1] + bias_ref[at]

    pre = [jax.nn.sigmoid(scaled(0, k)) for k in range(STREAMS)]
    columns[...] = jnp.concatenate(pre + [jnp.zeros((LANES - STREAMS, tokens), jnp.float32)]).T

    def input_copy(way, hop, i, origin):
        at = (pl.ds(origin * own_blocks, own_blocks), pl.ds(pl.multiple_of(i * tile, tile), tile), slice(None))
        return pltpu.make_async_remote_copy(
            src_ref=blocks.at[at],
            dst_ref=blocks.at[at],
            send_sem=input_send.at[way, hop],
            recv_sem=input_recv.at[way, hop, i],
            device_id=(s, z + 1 - 2 * way),
            device_id_type=MESH,
        )

    def passes(way, hop):
        if way == 0:
            return jnp.logical_and(z >= hop, z + 1 < n_tensor)
        return jnp.logical_and(z + hop < n_tensor, z >= 1)

    def gets(way, hop):
        return z - 1 - hop >= 0 if way == 0 else z + 1 + hop < n_tensor

    def input_start(way, hop, i):
        @pl.when(passes(way, hop))
        def _():
            input_copy(way, hop, i, z - hop if way == 0 else z + hop).start()

    def input_wait(way, hop, i):
        @pl.when(gets(way, hop))
        def _():
            input_copy(way, hop, i, z - 1 - hop if way == 0 else z + 1 + hop).wait_recv()

    @pl.loop(0, n_tiles)
    def _(i):
        for slot in (0, 1):
            tile_copy(i, slot).wait()
            at = pl.ds(pl.multiple_of(i * tile + slot * piece, piece), piece)
            weight = columns[at, :]
            mixed = 0.0
            for k in range(STREAMS):
                mixed += weight[:, k : k + 1] * tiles[slot, k]
            mixed = mixed.astype(jnp.bfloat16)
            for j in range(own_blocks):
                blocks[z * own_blocks + j, at, :] = mixed[:, j * block_width : (j + 1) * block_width]
            fetch(i + 1, slot)
        for way in (0, 1):
            input_start(way, 0, i)

    post = [2.0 * jax.nn.sigmoid(scaled(1, STREAMS + k)) for k in range(STREAMS)]
    start = tuple(jnp.exp(scaled(2, 2 * STREAMS + k)) for k in range(STREAMS * STREAMS))

    def balance(_, matrix):
        grid = [list(matrix[k * STREAMS : (k + 1) * STREAMS]) for k in range(STREAMS)]
        for k in range(STREAMS):
            row = grid[k][0] + grid[k][1] + grid[k][2] + grid[k][3]
            grid[k] = [g / row for g in grid[k]]
        for j in range(STREAMS):
            column = grid[0][j] + grid[1][j] + grid[2][j] + grid[3][j]
            for k in range(STREAMS):
                grid[k][j] = grid[k][j] / column
        return tuple(g for line in grid for g in line)

    res = lax.fori_loop(0, SWEEPS, balance, start)
    filler = LANES - STREAMS - STREAMS * STREAMS
    coef_ref[...] = jnp.concatenate(post + list(res) + [jnp.zeros((filler, tokens), jnp.float32)]).T

    for hop in range(n_tensor - 2):

        @pl.loop(0, n_tiles)
        def _(i):
            for way in (0, 1):
                input_wait(way, hop, i)
                input_start(way, hop + 1, i)

    @pl.loop(0, n_gate)
    def _(c):
        for r in range(1, last):
            gate_arrival(c, r)
            for o in stages[r]:
                for kind in (0, 1):
                    for t in children(o, orders[kind]):
                        gate_copy(kind, c, t).start()

    for c in range(n_down):
        for kind in (0, 1):
            for o in sorted(children(0, orders[kind]), key=lambda t: -t):
                down_copy(kind, c, o).start()
            down_copy_local(kind, c).start()

    granule = min(rows, block_width)

    @pl.loop(0, n_tiles)
    def _(i):
        at = pl.ds(pl.multiple_of(i * tile, tile), tile)
        for way in (0, 1):
            input_wait(way, n_tensor - 2, i)
        square = 0.0
        for j in range(n_tensor * own_blocks):
            value = blocks[j, at, :].astype(jnp.float32)
            square += value * value
        inverse = lax.rsqrt(jnp.sum(square, axis=1, keepdims=True) / features + EPSILON)
        for src in range(n_seq):
            o = flip(s, src)
            for g in range(rows // granule):
                col = src * rows + g * granule
                part = pl.ds(col % block_width, granule)
                value = blocks[col // block_width, at, part].astype(jnp.float32)
                value = value * inverse * gain_ref[pl.ds(col, granule)].astype(jnp.float32)[None, :]
                to = pl.ds(pl.multiple_of(o * rows + g * granule, LANES), granule)
                normed[at, to] = value.astype(jnp.bfloat16)

    for kind in (0, 1):
        await_bytes(weights[kind][1].at[:, pl.ds(0, rows), :], weight_local.at[kind])

    @pl.loop(0, n_gate)
    def _(c):
        gate_arrival(c, last)
        for kind in (0, 1):
            gate_copy(kind, c, everything + 1).start()
        await_bytes(gate_buf.at[c], weight_pair.at[c])
        gate_value = jnp.dot(normed[...], gate_buf[c], preferred_element_type=jnp.float32)
        up_value = jnp.dot(normed[...], up_buf[c], preferred_element_type=jnp.float32)
        to = pl.ds(pl.multiple_of(c * gate_width, LANES), gate_width)
        hidden[:, to] = (gate_value / (1.0 + jnp.exp(-gate_value)) * up_value).astype(jnp.bfloat16)

    def has(way):
        return z + 1 < n_tensor if way == 0 else z >= 1

    for way in (0, 1):

        @pl.when(has(way))
        def _():
            pl.semaphore_signal(free.at[way], inc=1, device_id=(s, z + 1 - 2 * way), device_id_type=MESH)

    for hop in range(n_tensor - 1):
        for way in (0, 1):

            @pl.when(passes(way, hop))
            def _():
                await_bytes(blocks.at[pl.ds(0, own_blocks)], input_send.at[way, hop])

    for way in (0, 1):

        @pl.when(has(way))
        def _():
            pl.semaphore_wait(free.at[1 - way], 1)

    stretch = tokens // SPLITS

    def place(c, q):
        source = flip(s, 2 * q)
        to = lax.div(source, per)
        at = c * pair_blocks + lax.rem(lax.div(source, 2), pair_blocks)
        return to, at, to * own_blocks + at

    def landing(from_right, at, index, part):
        at_rows = pl.ds(part * stretch, stretch)
        if from_right:
            return arrived.at[at, at_rows, :], part_recv.at[n_tensor * own_blocks + at, part]
        to = pl.ds(pl.multiple_of(index * block_width, LANES), block_width)
        return normed.at[at_rows, to], part_recv.at[index, part]

    def part_copy(c, q, part, way, from_right):
        _, at, index = place(c, q)
        target, arrival = landing(from_right, at, index, part)
        return pltpu.make_async_remote_copy(
            src_ref=blocks.at[index, pl.ds(part * stretch, stretch), :],
            dst_ref=target,
            send_sem=part_send.at[0],
            recv_sem=arrival,
            device_id=(s, z + 1 - 2 * way),
            device_id_type=MESH,
        )

    def part_start(c, q, part):
        to = place(c, q)[0]

        @pl.when(to > z)
        def _():
            part_copy(c, q, part, 0, False).start()

        @pl.when(to == z - 1)
        def _():
            part_copy(c, q, part, 1, True).start()

        @pl.when(to < z - 1)
        def _():
            part_copy(c, q, part, 1, False).start()

    def upstream(to):
        return jnp.where(to > z, z, jnp.where(to < z, n_tensor - 1 - z, 0))

    def project(c, q):
        value = jnp.dot(hidden[...], down_buf[c, q], preferred_element_type=jnp.float32).astype(jnp.bfloat16)
        to, _, index = place(c, q)
        core = lax.rem(s, 2)
        blocks[index, :, pl.ds(pl.multiple_of(core * half, LANES), half)] = value[:, :half]
        blocks[index, :, pl.ds(pl.multiple_of((1 - core) * half, LANES), half)] = value[:, half:]

        first = upstream(to) == 0
        if late(c, q):
            first = jnp.logical_and(first, jnp.abs(to - z) > 1)

        @pl.when(first)
        def _():
            for part in range(SPLITS):
                part_start(c, q, part)

    def late(c, q):
        return q not in (0, everything // 2) and 2 * c >= n_down

    def send_late(c, q):
        to = place(c, q)[0]

        @pl.when(jnp.logical_and(upstream(to) == 0, jnp.abs(to - z) == 1))
        def _():
            for part in range(SPLITS):
                part_start(c, q, part)

    def relay(c, q, distance):
        to, _, index = place(c, q)

        @pl.when(upstream(to) == distance)
        def _():
            for part in range(SPLITS):
                part_copy(c, q, part, 0, False).wait_recv()

                @pl.loop(0, stretch // piece)
                def _(i):
                    at = pl.ds(pl.multiple_of(part * stretch + i * piece, piece), piece)
                    incoming = normed[at, pl.ds(pl.multiple_of(index * block_width, LANES), block_width)]
                    value = blocks[index, at, :].astype(jnp.float32) + incoming.astype(jnp.float32)
                    blocks[index, at, :] = value.astype(jnp.bfloat16)

                part_start(c, q, part)

    groups = [[(c, 0) for c in range(n_down)]]
    groups += [[(c, o // 2) for r in range(1, last) for o in stages[r]] for c in range(n_down)]
    groups += [[(c, everything // 2)] for c in range(n_down)]
    due = {}

    def plan(step, group, distance):
        due.setdefault(group, []).append((distance, step))

    for c in range(n_down):
        for distance in range(1, n_tensor - 1):
            plan((c, 0), 1 + (c + 1) // 2 + distance - 1, distance)
            for step in groups[1 + c]:
                plan(step, 3 + c + (distance - 1) + (1 if 2 * c >= n_down else 0) + (1 if c > 0 and distance > 1 else 0), distance)
            plan((c, everything // 2), n_down + 3 + c + (distance - 1), distance)

    def relays(group):
        for distance, step in sorted(due.get(group, []), key=lambda entry: (-entry[0], entry[1][0])):
            relay(*step, distance)

    await_bytes(down_buf.at[:, 0, :, pl.ds(0, half)], down_local.at[0])
    for c, q in groups[0]:
        down_pair_arrival(c, 0)
        project(c, q)
    for c in range(n_down):
        for r in range(1, last):
            down_arrival(c, r)
            for o in stages[r]:
                for kind in (0, 1):
                    for t in children(o, orders[kind]):
                        down_copy(kind, c, t).start()
        for r in range(1, last):
            down_pair_arrival(c, r)
            for o in stages[r]:
                project(c, o // 2)
        relays(1 + c)
    for c in range(n_down):
        down_arrival(c, last)
        for kind in (0, 1):
            down_copy(kind, c, everything + 1).start()
        down_pair_arrival(c, last)
        project(c, everything // 2)
        if c == n_down - 1:
            for group in groups:
                for step in group:
                    if late(*step):
                        send_late(*step)
        relays(1 + n_down + c)
    for group in range(1 + 2 * n_down, max(due) + 1):
        relays(group)

    for at in range(own_blocks):
        c, p = at // pair_blocks, at % pair_blocks
        index = z * own_blocks + at
        columns_of = [pl.ds((2 * p + h) * rows + c * half, half) for h in (0, 1)]
        for h in (0, 1):
            out_ref[:, columns_of[h]] = blocks[index, :, pl.ds(h * half, half)].astype(jnp.float32)
        for from_right in (False, True):

            @pl.when(has(0 if from_right else 1))
            def _():
                for part in range(SPLITS):
                    target, arrival = landing(from_right, at, index, part)
                    pltpu.make_async_remote_copy(
                        src_ref=blocks.at[index, pl.ds(part * stretch, stretch), :],
                        dst_ref=target,
                        send_sem=part_send.at[0],
                        recv_sem=arrival,
                        device_id=(s, z + 1 if from_right else z - 1),
                        device_id_type=MESH,
                    ).wait_recv()
                    at_rows = pl.ds(part * stretch, stretch)
                    for h in (0, 1):
                        if from_right:
                            value = arrived[at, at_rows, pl.ds(h * half, half)]
                        else:
                            to = pl.ds(pl.multiple_of(index * block_width + h * half, LANES), half)
                            value = normed[at_rows, to]
                        out_ref[at_rows, columns_of[h]] += value.astype(jnp.float32)

    await_bytes(stats.at[pl.ds(1, n_tensor - 1)], stat_send.at[0])
    for kind in (0, 1):
        await_bytes(weights[kind][1].at[:, pl.ds(rows, (n_seq - 1) * rows), :], weight_send.at[kind])
    await_bytes(down_buf.at[:, pl.ds(0, pairs - 1), :, pl.ds(0, half)], down_send.at[0])
    await_bytes(down_buf.at[:, :, :, pl.ds(0, half)], down_send.at[1])
    await_bytes(blocks.at[pl.ds(0, (n_tensor - 1) * own_blocks)], part_send.at[0])


def feed_forward(mesh, streams, mix_weight, mix_bias, mix_scale, norm_gain, gate_weight, up_weight, down_weight):
    n_seq, n_tensor = mesh.shape["seq"], mesh.shape["tensor"]
    tokens, width = streams.shape[1:]
    units = gate_weight.shape[1]
    rows = gate_weight.shape[0]
    features = width * n_tensor
    gate_width = width_of(units, 2 * LANES)
    n_gate = units // gate_width
    half = LANES
    n_down = down_weight.shape[1] // half
    own_blocks = width // (2 * half)
    tile = LANES
    n_tiles = tokens // tile
    exchanges = int(math.log2(n_seq)) - 1
    hbm, vmem = pl.BlockSpec(memory_space=pl.ANY), pl.BlockSpec(memory_space=pltpu.VMEM)
    smem = pl.BlockSpec(memory_space=pltpu.SMEM)
    dma = pltpu.SemaphoreType.DMA
    return pl.pallas_call(
        functools.partial(block_kernel, n_seq, n_tensor),
        out_shape=(
            jax.ShapeDtypeStruct((tokens, width), jnp.float32),
            jax.ShapeDtypeStruct((tokens, LANES), jnp.float32),
        ),
        in_specs=[smem, smem, vmem, vmem, hbm, hbm, hbm, hbm],
        out_specs=(vmem, vmem),
        scratch_shapes=[
            pltpu.VMEM((n_gate, n_seq * rows, gate_width), jnp.bfloat16),
            pltpu.VMEM((n_gate, n_seq * rows, gate_width), jnp.bfloat16),
            pltpu.VMEM((n_down, n_seq // 2, units, 2 * half), jnp.bfloat16),
            pltpu.VMEM((n_tensor * own_blocks, tokens, 2 * half), jnp.bfloat16),
            pltpu.VMEM((tokens, features), jnp.bfloat16),
            pltpu.VMEM((tokens, units), jnp.bfloat16),
            pltpu.VMEM((own_blocks, tokens, 2 * half), jnp.bfloat16),
            pltpu.VMEM((2, STREAMS, tile // 2, width), jnp.float32),
            pltpu.VMEM((STREAMS, 2 * mix_weight.shape[0], width), jnp.bfloat16),
            pltpu.VMEM((n_tensor, mix_weight.shape[0] + 8, tokens), jnp.float32),
            pltpu.VMEM((tokens, LANES), jnp.float32),
            dma((2,)),
            dma((2,)),
            dma((2,)),
            dma((n_gate, exchanges)),
            dma((n_gate,)),
            dma((2,)),
            dma((1,)),
            dma((n_down, exchanges)),
            dma((n_down, exchanges + 1)),
            dma((1,)),
            dma((1,)),
            dma((2, n_tensor - 1)),
            dma((2, n_tensor - 1, n_tiles)),
            dma((1,)),
            dma(((n_tensor + 1) * own_blocks, SPLITS)),
            pltpu.SemaphoreType.REGULAR((2,)),
        ],
        compiler_params=pltpu.CompilerParams(
            collective_id=0, has_side_effects=True, vmem_limit_bytes=67_043_328
        ),
    )(mix_bias, mix_scale, mix_weight, norm_gain, streams, gate_weight, up_weight, down_weight)


def mix_kernel(streams_ref, layer_ref, mix_ref, out_ref, streams, layer, mixes, mixed, in_sem, out_sem):
    tile = layer.shape[0] // MIX_TILES

    def rows_of(i):
        return pl.ds(pl.multiple_of(i * tile, tile), tile)

    def incoming(i):
        at = rows_of(i)
        return (
            pltpu.make_async_copy(mix_ref.at[at, :], mixes.at[at, :], in_sem.at[0, i]),
            pltpu.make_async_copy(layer_ref.at[at, :], layer.at[at, :], in_sem.at[1, i]),
            pltpu.make_async_copy(streams_ref.at[:, at, :], streams.at[:, at, :], in_sem.at[2, i]),
        )

    for i in range(MIX_TILES):
        for copy in incoming(i):
            copy.start()

    @pl.loop(0, MIX_TILES)
    def _(i):
        for copy in incoming(i):
            copy.wait()

        @pl.loop(0, tile // SUBLANES, unroll=4)
        def _(j):
            at = pl.ds(pl.multiple_of(i * tile + j * SUBLANES, SUBLANES), SUBLANES)
            layer_out = layer[at, :]
            weight = mixes[at, :]
            current = [streams[source, at, :] for source in range(STREAMS)]
            for target in range(STREAMS):
                value = weight[:, target : target + 1] * layer_out
                for source in range(STREAMS):
                    column = STREAMS * (1 + target) + source
                    value = value + weight[:, column : column + 1] * current[source]
                mixed[target, at, :] = value

        at = rows_of(i)
        pltpu.make_async_copy(mixed.at[:, at, :], out_ref.at[:, at, :], out_sem.at[0]).start()

    pltpu.make_async_copy(mixed, out_ref, out_sem.at[0]).wait()


def mix_streams(streams, layer_out, mixes):
    hbm = pl.BlockSpec(memory_space=pl.ANY)
    return pl.pallas_call(
        mix_kernel,
        in_specs=[hbm] * 3,
        out_specs=hbm,
        out_shape=jax.ShapeDtypeStruct(streams.shape, jnp.float32),
        scratch_shapes=[
            pltpu.VMEM(streams.shape, jnp.float32),
            pltpu.VMEM(layer_out.shape, jnp.float32),
            pltpu.VMEM(mixes.shape, jnp.float32),
            pltpu.VMEM(streams.shape, jnp.float32),
            pltpu.SemaphoreType.DMA((3, MIX_TILES)),
            pltpu.SemaphoreType.DMA((1,)),
        ],
        compiler_params=pltpu.CompilerParams(vmem_limit_bytes=67_043_328),
    )(streams, layer_out, mixes)


def solution(mesh):
    def body(streams, *rest):
        layer_out, mixes = feed_forward(mesh, streams, *rest)
        return mix_streams(streams, layer_out, mixes)

    placed = (
        P(None, "seq", "tensor"),
        P(None, None, "tensor"),
        P(),
        P(),
        P(),
        P("seq", "tensor"),
        P("seq", "tensor"),
        P("tensor", "seq"),
    )
    return jax.shard_map(body, mesh=mesh, in_specs=placed, out_specs=P(None, "seq", "tensor"), check_vma=False)
```

```python
import functools
import math

import jax
import jax.numpy as jnp
from jax import lax
from jax.experimental import pallas as pl
from jax.experimental.pallas import tpu as pltpu
from jax.sharding import PartitionSpec as P

STREAMS = 4
SWEEPS = 20
EPSILON = 0.25
LANES = 128
SUBLANES = 8
SPLITS = 2
MIX_TILES = 8
AHEAD = 2
MESH = pl.DeviceIdType.MESH
HIGHEST = lax.Precision.HIGHEST


def flip(index, offset):
    bit, out = 1, index
    while bit <= offset:
        if offset & bit:
            out = out + bit - 2 * bit * lax.rem(lax.div(index, bit), 2)
        bit *= 2
    return out


def last_bit(offset, order):
    if offset & 1:
        return 1
    return [b for b in order if offset & b][-1]


def width_of(size, limit):
    width = limit
    while size % width:
        width -= LANES
    return width


def plan_relays(n_seq, n_tensor, n_down, stages):
    hop, latency, unit, product = 5.6, 1.7, 9.8, 1.15
    last = len(stages) - 1
    middle = [o // 2 for r in range(1, last) for o in stages[r]]
    groups = []
    now = 0.0
    starts, ends = [], []

    def add(c, r, blocks_of, arrival):
        nonlocal now
        starts.append(max(now, arrival))
        now = starts[-1] + product * len(blocks_of)
        groups.append((c, r, blocks_of))
        ends.append(now)

    for c in range(n_down):
        add(c, 0, [0], 0.0)
    queue = [("own", c) for c in range(min(AHEAD, n_down))]
    for c in range(n_down):
        queue.append(("pass", c))
        if c + AHEAD < n_down:
            queue.append(("own", c + AHEAD))
    clock = 6.5 - unit
    for what, c in queue:
        clock += unit if what == "own" else unit / 2
        if what == "own":
            add(c, last - 1, middle, clock + 1.5)
        else:
            add(c, last, [stages[last][0] // 2], clock + 1.5)
    home = {(c, q): g for g, (c, _, blocks_of) in enumerate(groups) for q in blocks_of}
    final = len(groups) - 1

    def end(g):
        return ends[g] if g <= final else ends[final] + 2.0 * (g - final)

    def until(g):
        return starts[g + 1] - 1.0 if g < final else end(g)

    per = n_seq // n_tensor
    relayed, near = {}, {}
    for chip in range(n_seq // 2):
        for way in (1, -1):
            line = range(n_tensor) if way == 1 else range(n_tensor - 1, -1, -1)
            incoming = {}
            for place, z in enumerate(line):
                device = chip * n_tensor + z
                ahead = {step: (2 * (chip ^ step[1]) // per - z) * way for step in home}
                free_at, passed = 0.0, {}
                if place == 0:
                    held, sent = [], 0
                    for k in range(final + 1):
                        for step in [step for step, g in home.items() if g == k]:
                            if ahead[step] == 1:
                                held.append(step)
                            elif ahead[step] > 1:
                                free_at = max(free_at, ends[k]) + hop
                                passed[step] = (free_at + latency, k)
                        while held and (k == final or (sent < n_down - 1 and free_at < ends[k + 1])):
                            sent += 1
                            free_at = max(free_at, ends[k]) + hop
                            near.setdefault((k, held.pop(0)), []).append((free_at, device))
                else:
                    leaving = []
                    for step, g in home.items():
                        if ahead[step] <= 0:
                            continue
                        arrival, least = incoming[step]
                        k = max(g, least)
                        while max(until(k), end(k)) < arrival - 1.0:
                            k += 1
                        relayed.setdefault((k, step), []).append((arrival, device))
                        leaving.append((max(end(k), arrival), step, k))
                    for ready, step, k in sorted(leaving):
                        free_at = max(free_at, ready) + hop
                        passed[step] = (free_at + latency, k + 1)
                incoming = passed

    def by_group(found):
        plan = {}
        for (k, step), entries in sorted(found.items(), key=lambda item: min(item[1])[0]):
            plan.setdefault(k, []).append((step, sorted(d for _, d in entries)))
        return plan

    return groups, by_group(near), by_group(relayed)


def block_kernel(
    n_seq,
    n_tensor,
    bias_ref,
    scale_ref,
    mix_hbm,
    gain_ref,
    streams_ref,
    gate_ref,
    up_ref,
    down_ref,
    out_hbm,
    coef_hbm,
    mix_ref,
    out_ref,
    coef_ref,
    gate_buf,
    up_buf,
    down_buf,
    blocks,
    normed,
    hidden,
    arrived,
    tiles,
    mix_parts,
    stats,
    columns,
    tile_sem,
    weight_send,
    weight_local,
    weight_recv,
    weight_pair,
    down_send,
    down_local,
    down_recv,
    down_pair,
    stat_send,
    stat_recv,
    input_send,
    input_recv,
    part_send,
    part_recv,
    edge_sem,
    free,
):
    s, z = lax.axis_index("seq"), lax.axis_index("tensor")
    tokens, width = out_ref.shape
    features = width * n_tensor
    rows = features // n_seq
    n_gate, _, gate_width = gate_buf.shape
    n_down, pairs, units, block_width = down_buf.shape
    half = block_width // 2
    per = n_seq // n_tensor
    pair_blocks = per // 2
    own_blocks = n_down * pair_blocks
    piece = tiles.shape[2]
    tile = 2 * piece
    n_tiles = tokens // tile

    bits = []
    bit = 2
    while bit < n_seq:
        bits.append(bit)
        bit *= 2
    orders = (bits, bits[::-1])
    everything = n_seq - 2
    last = len(bits)

    def stage(o):
        return bin(o - o % 2).count("1")

    stages = [[o for o in range(0, n_seq, 2) if stage(o) == r] for r in range(last + 1)]

    def await_bytes(ref, sem):
        pltpu.make_async_copy(ref, ref, sem).wait()

    def peer(offset):
        return (flip(s, offset), z)

    def across(shift):
        return (s, lax.rem(z + shift, n_tensor))

    barrier = pltpu.get_barrier_semaphore()
    for b in [1] + bits:
        pl.semaphore_signal(barrier, inc=1, device_id=peer(b), device_id_type=MESH)
    for shift in range(1, n_tensor):
        pl.semaphore_signal(barrier, inc=1, device_id=across(shift), device_id_type=MESH)
    pl.semaphore_wait(barrier, len(bits) + n_tensor)

    weights = ((gate_ref, gate_buf), (up_ref, up_buf))

    def gate_slot(kind, c, o):
        return weights[kind][1].at[c, pl.ds(o * rows, rows), :]

    def gate_own(kind, c):
        return weights[kind][0].at[:, pl.ds(pl.multiple_of(c * gate_width, LANES), gate_width)]

    def gate_copy(kind, c, o):
        b = last_bit(o, orders[kind])
        source = gate_own(kind, c) if o == b else gate_slot(kind, c, o ^ b)
        return pltpu.make_async_remote_copy(
            src_ref=source,
            dst_ref=gate_slot(kind, c, o),
            send_sem=weight_send.at[kind],
            recv_sem=weight_pair.at[c] if o % 2 else weight_recv.at[c, stage(o) - 1],
            device_id=peer(b),
            device_id_type=MESH,
        )

    def gate_copy_local(kind, c):
        return pltpu.make_async_copy(gate_own(kind, c), gate_slot(kind, c, 0), weight_local.at[kind])

    def gate_arrival(c, r):
        await_bytes(gate_buf.at[c, pl.ds(0, 2 * len(stages[r]) * rows), :], weight_recv.at[c, r - 1])

    depth = units // 2

    def down_slot(kind, c, o):
        return down_buf.at[c, o // 2, pl.ds(kind * depth, depth), pl.ds((o % 2) * half, half)]

    def down_own(kind, c):
        return down_ref.at[pl.ds(kind * depth, depth), pl.ds(pl.multiple_of(c * half, LANES), half)]

    def down_copy(kind, c, o):
        b = last_bit(o, orders[kind])
        return pltpu.make_async_remote_copy(
            src_ref=down_own(kind, c) if o == b else down_slot(kind, c, o ^ b),
            dst_ref=down_slot(kind, c, o),
            send_sem=down_send.at[o % 2],
            recv_sem=down_pair.at[c, stage(o)] if o % 2 else down_recv.at[c, stage(o) - 1],
            device_id=peer(b),
            device_id_type=MESH,
        )

    def down_copy_local(kind, c):
        return pltpu.make_async_copy(down_own(kind, c), down_slot(kind, c, 0), down_local.at[c])

    def down_share(c, r):
        return down_buf.at[c, pl.ds(0, len(stages[r])), :, pl.ds(0, half)]

    def down_arrival(c, r):
        await_bytes(down_share(c, r), down_recv.at[c, r - 1])

    def down_pair_arrival(c, r):
        await_bytes(down_share(c, r), down_pair.at[c, r])

    def children(o, order):
        return [t for t in range(1, n_seq) if t ^ last_bit(t, order) == o and t != o]

    @pl.loop(0, n_gate)
    def _(c):
        for kind in (0, 1):
            for o in sorted(children(0, orders[kind]), key=lambda t: -t):
                gate_copy(kind, c, o).start()
            gate_copy_local(kind, c).start()

    mix_in = pltpu.make_async_copy(mix_hbm, mix_ref, edge_sem.at[0])
    coef_out = pltpu.make_async_copy(coef_ref, coef_hbm, edge_sem.at[1])
    mix_in.start()

    def tile_copy(i, slot):
        at = pl.ds(pl.multiple_of(i * tile + slot * piece, piece), piece)
        return pltpu.make_async_copy(streams_ref.at[:, at, :], tiles.at[slot], tile_sem.at[slot])

    def fetch(i, slot):
        @pl.when(i < n_tiles)
        def _():
            tile_copy(i, slot).start()

    for slot in (0, 1):
        tile_copy(0, slot).start()

    def halves(value):
        high = value.astype(jnp.bfloat16)
        return high, (value - high.astype(jnp.float32)).astype(jnp.bfloat16)

    n_logits = mix_ref.shape[0]
    mix_in.wait()
    for k in range(STREAMS):
        mix_parts[k] = jnp.concatenate(halves(mix_ref[:, k, :]))

    @pl.loop(0, n_tiles)
    def _(i):
        contract = (((1,), (1,)), ((), ()))
        found = []
        for slot in (0, 1):
            tile_copy(i, slot).wait()
            product = square = 0.0
            for k in range(STREAMS):
                current = tiles[slot, k]
                product += lax.dot_general(
                    mix_parts[k], jnp.concatenate(halves(current)), contract, preferred_element_type=jnp.float32
                )
                square += current * current
            product = product[:n_logits] + product[n_logits:]
            logits = product[:, :piece] + product[:, piece:]
            square = sum(square[:, j : j + LANES] for j in range(0, width, LANES))
            squares = lax.dot_general(
                jnp.ones((8, LANES), jnp.float32),
                square,
                contract,
                precision=HIGHEST,
                preferred_element_type=jnp.float32,
            )
            found.append(jnp.concatenate([logits, squares]))
            fetch(i + 1, slot)
        stats[0, :, pl.ds(pl.multiple_of(i * tile, LANES), tile)] = jnp.concatenate(found, axis=1)

    def stat_copy(shift):
        return pltpu.make_async_remote_copy(
            src_ref=stats.at[0],
            dst_ref=stats.at[shift],
            send_sem=stat_send.at[0],
            recv_sem=stat_recv.at[0],
            device_id=across(shift),
            device_id_type=MESH,
        )

    for shift in range(1, n_tensor):
        stat_copy(shift).start()
    for slot in (0, 1):
        tile_copy(0, slot).start()
    await_bytes(stats.at[pl.ds(1, n_tensor - 1)], stat_recv.at[0])
    total = stats[0]
    for shift in range(1, n_tensor):
        total = total + stats[shift]
    logits = total[:n_logits] * lax.rsqrt(total[n_logits : n_logits + 1] / (STREAMS * features) + EPSILON)

    def scaled(which, at):
        return scale_ref[which] * logits[at : at + 1] + bias_ref[at]

    pre = [jax.nn.sigmoid(scaled(0, k)) for k in range(STREAMS)]
    columns[...] = jnp.concatenate(pre + [jnp.zeros((LANES - STREAMS, tokens), jnp.float32)]).T

    def input_copy(way, hop, i, origin):
        at = (pl.ds(origin * own_blocks, own_blocks), pl.ds(pl.multiple_of(i * tile, tile), tile), slice(None))
        return pltpu.make_async_remote_copy(
            src_ref=blocks.at[at],
            dst_ref=blocks.at[at],
            send_sem=input_send.at[way, hop],
            recv_sem=input_recv.at[way, hop, i],
            device_id=(s, z + 1 - 2 * way),
            device_id_type=MESH,
        )

    def passes(way, hop):
        if way == 0:
            return jnp.logical_and(z >= hop, z + 1 < n_tensor)
        return jnp.logical_and(z + hop < n_tensor, z >= 1)

    def gets(way, hop):
        return z - 1 - hop >= 0 if way == 0 else z + 1 + hop < n_tensor

    def input_start(way, hop, i):
        @pl.when(passes(way, hop))
        def _():
            input_copy(way, hop, i, z - hop if way == 0 else z + hop).start()

    def input_wait(way, hop, i):
        @pl.when(gets(way, hop))
        def _():
            input_copy(way, hop, i, z - 1 - hop if way == 0 else z + 1 + hop).wait_recv()

    @pl.loop(0, n_tiles)
    def _(i):
        for slot in (0, 1):
            tile_copy(i, slot).wait()
            at = pl.ds(pl.multiple_of(i * tile + slot * piece, piece), piece)
            weight = columns[at, :]
            mixed = 0.0
            for k in range(STREAMS):
                mixed += weight[:, k : k + 1] * tiles[slot, k]
            mixed = mixed.astype(jnp.bfloat16)
            for j in range(own_blocks):
                blocks[z * own_blocks + j, at, :] = mixed[:, j * block_width : (j + 1) * block_width]
            fetch(i + 1, slot)
        for way in (0, 1):
            input_start(way, 0, i)

    post = [2.0 * jax.nn.sigmoid(scaled(1, STREAMS + k)) for k in range(STREAMS)]
    start = tuple(jnp.exp(scaled(2, 2 * STREAMS + k)) for k in range(STREAMS * STREAMS))

    def balance(_, matrix):
        grid = [list(matrix[k * STREAMS : (k + 1) * STREAMS]) for k in range(STREAMS)]
        for k in range(STREAMS):
            row = grid[k][0] + grid[k][1] + grid[k][2] + grid[k][3]
            grid[k] = [g / row for g in grid[k]]
        for j in range(STREAMS):
            column = grid[0][j] + grid[1][j] + grid[2][j] + grid[3][j]
            for k in range(STREAMS):
                grid[k][j] = grid[k][j] / column
        return tuple(g for line in grid for g in line)

    res = lax.fori_loop(0, SWEEPS, balance, start)
    filler = LANES - STREAMS - STREAMS * STREAMS
    coef_ref[...] = jnp.concatenate(post + list(res) + [jnp.zeros((filler, tokens), jnp.float32)]).T

    coef_out.start()

    for hop in range(n_tensor - 2):

        @pl.loop(0, n_tiles)
        def _(i):
            for way in (0, 1):
                input_wait(way, hop, i)
                input_start(way, hop + 1, i)

    @pl.loop(0, n_gate)
    def _(c):
        for r in range(1, last):
            gate_arrival(c, r)
            for o in stages[r]:
                for kind in (0, 1):
                    for t in children(o, orders[kind]):
                        gate_copy(kind, c, t).start()

    def down_leave(c):
        for kind in (0, 1):
            for o in sorted(children(0, orders[kind]), key=lambda t: -t):
                if o != 1:
                    down_copy(kind, c, o).start()

    for c in range(n_down):
        for kind in (0, 1):
            down_copy(kind, c, 1).start()
            down_copy_local(kind, c).start()
    for c in range(min(AHEAD, n_down)):
        down_leave(c)

    granule = min(rows, block_width)

    @pl.loop(0, n_tiles)
    def _(i):
        at = pl.ds(pl.multiple_of(i * tile, tile), tile)
        for way in (0, 1):
            input_wait(way, n_tensor - 2, i)
        square = 0.0
        for j in range(n_tensor * own_blocks):
            value = blocks[j, at, :].astype(jnp.float32)
            square += value * value
        inverse = lax.rsqrt(jnp.sum(square, axis=1, keepdims=True) / features + EPSILON)
        for src in range(n_seq):
            o = flip(s, src)
            for g in range(rows // granule):
                col = src * rows + g * granule
                part = pl.ds(col % block_width, granule)
                value = blocks[col // block_width, at, part].astype(jnp.float32)
                value = value * inverse * gain_ref[pl.ds(col, granule)].astype(jnp.float32)[None, :]
                to = pl.ds(pl.multiple_of(o * rows + g * granule, LANES), granule)
                normed[at, to] = value.astype(jnp.bfloat16)

    for kind in (0, 1):
        await_bytes(weights[kind][1].at[:, pl.ds(0, rows), :], weight_local.at[kind])

    @pl.loop(0, n_gate)
    def _(c):
        gate_arrival(c, last)
        for kind in (0, 1):
            gate_copy(kind, c, everything + 1).start()
        await_bytes(gate_buf.at[c], weight_pair.at[c])
        gate_value = jnp.dot(normed[...], gate_buf[c], preferred_element_type=jnp.float32)
        up_value = jnp.dot(normed[...], up_buf[c], preferred_element_type=jnp.float32)
        to = pl.ds(pl.multiple_of(c * gate_width, LANES), gate_width)
        hidden[:, to] = (gate_value / (1.0 + jnp.exp(-gate_value)) * up_value).astype(jnp.bfloat16)

    def has(way):
        return z + 1 < n_tensor if way == 0 else z >= 1

    for way in (0, 1):

        @pl.when(has(way))
        def _():
            pl.semaphore_signal(free.at[way], inc=1, device_id=(s, z + 1 - 2 * way), device_id_type=MESH)

    for hop in range(n_tensor - 1):
        for way in (0, 1):

            @pl.when(passes(way, hop))
            def _():
                await_bytes(blocks.at[pl.ds(0, own_blocks)], input_send.at[way, hop])

    for way in (0, 1):

        @pl.when(has(way))
        def _():
            pl.semaphore_wait(free.at[1 - way], 1)

    stretch = tokens // SPLITS

    def place(c, q):
        source = flip(s, 2 * q)
        to = lax.div(source, per)
        at = c * pair_blocks + lax.rem(lax.div(source, 2), pair_blocks)
        return to, at, to * own_blocks + at

    def landing(from_right, at, index, part):
        at_rows = pl.ds(part * stretch, stretch)
        if from_right:
            return arrived.at[at, at_rows, :], part_recv.at[n_tensor * own_blocks + at, part]
        to = pl.ds(pl.multiple_of(index * block_width, LANES), block_width)
        return normed.at[at_rows, to], part_recv.at[index, part]

    def part_copy(c, q, part, way, from_right):
        _, at, index = place(c, q)
        target, arrival = landing(from_right, at, index, part)
        return pltpu.make_async_remote_copy(
            src_ref=blocks.at[index, pl.ds(part * stretch, stretch), :],
            dst_ref=target,
            send_sem=part_send.at[0],
            recv_sem=arrival,
            device_id=(s, z + 1 - 2 * way),
            device_id_type=MESH,
        )

    def part_start(c, q, part):
        to = place(c, q)[0]

        @pl.when(to > z)
        def _():
            part_copy(c, q, part, 0, False).start()

        @pl.when(to == z - 1)
        def _():
            part_copy(c, q, part, 1, True).start()

        @pl.when(to < z - 1)
        def _():
            part_copy(c, q, part, 1, False).start()

    def upstream(to):
        return jnp.where(to > z, z, jnp.where(to < z, n_tensor - 1 - z, 0))

    def project(c, q):
        value = jnp.dot(hidden[...], down_buf[c, q], preferred_element_type=jnp.float32).astype(jnp.bfloat16)
        to, _, index = place(c, q)
        core = lax.rem(s, 2)
        blocks[index, :, pl.ds(pl.multiple_of(core * half, LANES), half)] = value[:, :half]
        blocks[index, :, pl.ds(pl.multiple_of((1 - core) * half, LANES), half)] = value[:, half:]

        @pl.when(jnp.logical_and(upstream(to) == 0, jnp.abs(to - z) > 1))
        def _():
            for part in range(SPLITS):
                part_start(c, q, part)

    def relay(c, q):
        index = place(c, q)[2]

        @pl.loop(0, SPLITS)
        def _(part):
            part_copy(c, q, part, 0, False).wait_recv()

            @pl.loop(0, stretch // piece)
            def _(i):
                at = pl.ds(pl.multiple_of(part * stretch + i * piece, piece), piece)
                incoming = normed[at, pl.ds(pl.multiple_of(index * block_width, LANES), block_width)]
                value = blocks[index, at, :].astype(jnp.float32) + incoming.astype(jnp.float32)
                blocks[index, at, :] = value.astype(jnp.bfloat16)

            part_start(c, q, part)

    groups, near, due = plan_relays(n_seq, n_tensor, n_down, stages)
    device = lax.div(s, 2) * n_tensor + z

    def one_of(devices):
        return functools.reduce(jnp.logical_or, [device == d for d in devices])

    def send_near(group, steps):
        for (c, q), devices in near.get(group, []):
            if (c, q) in steps:

                @pl.when(one_of(devices))
                def _():
                    for part in range(SPLITS):
                        part_start(c, q, part)

    def relays(group):
        for (c, q), devices in due.get(group, []):

            @pl.when(one_of(devices))
            def _():
                relay(c, q)

    for group, (c, r, blocks_of) in enumerate(groups):
        if r > 0:
            first = range(1, last) if r < last else (last,)
            for level in first:
                down_arrival(c, level)
                for o in stages[level]:
                    for kind in (0, 1):
                        for t in children(o, orders[kind]):
                            down_copy(kind, c, t).start()
            if r < last and c + AHEAD < n_down:
                down_leave(c + AHEAD)
            for level in first:
                down_pair_arrival(c, level)
        else:
            await_bytes(down_buf.at[c, 0, :, pl.ds(0, half)], down_local.at[c])
            down_pair_arrival(c, 0)
        for q in blocks_of:
            project(c, q)
            send_near(group, [(c, q)])
        send_near(group, [step for step, _ in near.get(group, []) if step not in [(c, q) for q in blocks_of]])
        relays(group)
    for group in range(len(groups), max(due, default=-1) + 1):
        relays(group)

    for at in range(own_blocks):
        c, p = at // pair_blocks, at % pair_blocks
        index = z * own_blocks + at
        columns_of = [pl.ds((2 * p + h) * rows + c * half, half) for h in (0, 1)]
        for h in (0, 1):
            out_ref[:, columns_of[h]] = blocks[index, :, pl.ds(h * half, half)].astype(jnp.float32)
        for from_right in (False, True):

            @pl.when(has(0 if from_right else 1))
            def _():
                for part in range(SPLITS):
                    target, arrival = landing(from_right, at, index, part)
                    pltpu.make_async_remote_copy(
                        src_ref=blocks.at[index, pl.ds(part * stretch, stretch), :],
                        dst_ref=target,
                        send_sem=part_send.at[0],
                        recv_sem=arrival,
                        device_id=(s, z + 1 if from_right else z - 1),
                        device_id_type=MESH,
                    ).wait_recv()
                    at_rows = pl.ds(part * stretch, stretch)
                    for h in (0, 1):
                        if from_right:
                            value = arrived[at, at_rows, pl.ds(h * half, half)]
                        else:
                            to = pl.ds(pl.multiple_of(index * block_width + h * half, LANES), half)
                            value = normed[at_rows, to]
                        out_ref[at_rows, columns_of[h]] += value.astype(jnp.float32)

        for h in (0, 1):
            pltpu.make_async_copy(out_ref.at[:, columns_of[h]], out_hbm.at[:, columns_of[h]], edge_sem.at[2]).start()

    coef_out.wait()
    await_bytes(out_ref, edge_sem.at[2])
    await_bytes(stats.at[pl.ds(1, n_tensor - 1)], stat_send.at[0])
    for kind in (0, 1):
        await_bytes(weights[kind][1].at[:, pl.ds(rows, (n_seq - 1) * rows), :], weight_send.at[kind])
    await_bytes(down_buf.at[:, pl.ds(0, pairs - 1), :, pl.ds(0, half)], down_send.at[0])
    await_bytes(down_buf.at[:, :, :, pl.ds(0, half)], down_send.at[1])
    await_bytes(blocks.at[pl.ds(0, (n_tensor - 1) * own_blocks)], part_send.at[0])


def feed_forward(mesh, streams, mix_weight, mix_bias, mix_scale, norm_gain, gate_weight, up_weight, down_weight):
    n_seq, n_tensor = mesh.shape["seq"], mesh.shape["tensor"]
    tokens, width = streams.shape[1:]
    units = gate_weight.shape[1]
    rows = gate_weight.shape[0]
    features = width * n_tensor
    gate_width = width_of(units, 2 * LANES)
    n_gate = units // gate_width
    half = LANES
    n_down = down_weight.shape[1] // half
    own_blocks = width // (2 * half)
    tile = LANES
    n_tiles = tokens // tile
    exchanges = int(math.log2(n_seq)) - 1
    hbm, vmem = pl.BlockSpec(memory_space=pl.ANY), pl.BlockSpec(memory_space=pltpu.VMEM)
    smem = pl.BlockSpec(memory_space=pltpu.SMEM)
    dma = pltpu.SemaphoreType.DMA
    return pl.pallas_call(
        functools.partial(block_kernel, n_seq, n_tensor),
        out_shape=(
            jax.ShapeDtypeStruct((tokens, width), jnp.float32),
            jax.ShapeDtypeStruct((tokens, LANES), jnp.float32),
        ),
        in_specs=[smem, smem, hbm, vmem, hbm, hbm, hbm, hbm],
        out_specs=(hbm, hbm),
        scratch_shapes=[
            pltpu.VMEM(mix_weight.shape, jnp.float32),
            pltpu.VMEM((tokens, width), jnp.float32),
            pltpu.VMEM((tokens, LANES), jnp.float32),
            pltpu.VMEM((n_gate, n_seq * rows, gate_width), jnp.bfloat16),
            pltpu.VMEM((n_gate, n_seq * rows, gate_width), jnp.bfloat16),
            pltpu.VMEM((n_down, n_seq // 2, units, 2 * half), jnp.bfloat16),
            pltpu.VMEM((n_tensor * own_blocks, tokens, 2 * half), jnp.bfloat16),
            pltpu.VMEM((tokens, features), jnp.bfloat16),
            pltpu.VMEM((tokens, units), jnp.bfloat16),
            pltpu.VMEM((own_blocks, tokens, 2 * half), jnp.bfloat16),
            pltpu.VMEM((2, STREAMS, tile // 2, width), jnp.float32),
            pltpu.VMEM((STREAMS, 2 * mix_weight.shape[0], width), jnp.bfloat16),
            pltpu.VMEM((n_tensor, mix_weight.shape[0] + 8, tokens), jnp.float32),
            pltpu.VMEM((tokens, LANES), jnp.float32),
            dma((2,)),
            dma((2,)),
            dma((2,)),
            dma((n_gate, exchanges)),
            dma((n_gate,)),
            dma((2,)),
            dma((n_down,)),
            dma((n_down, exchanges)),
            dma((n_down, exchanges + 1)),
            dma((1,)),
            dma((1,)),
            dma((2, n_tensor - 1)),
            dma((2, n_tensor - 1, n_tiles)),
            dma((1,)),
            dma(((n_tensor + 1) * own_blocks, SPLITS)),
            dma((3,)),
            pltpu.SemaphoreType.REGULAR((2,)),
        ],
        compiler_params=pltpu.CompilerParams(
            collective_id=0, has_side_effects=True, vmem_limit_bytes=67_043_328
        ),
    )(mix_bias, mix_scale, mix_weight, norm_gain, streams, gate_weight, up_weight, down_weight)


def mix_kernel(streams_ref, layer_ref, mix_ref, out_ref, streams, layer, mixes, mixed, in_sem, out_sem):
    tile = layer.shape[0] // MIX_TILES

    def rows_of(i):
        return pl.ds(pl.multiple_of(i * tile, tile), tile)

    def incoming(i):
        at = rows_of(i)
        return (
            pltpu.make_async_copy(mix_ref.at[at, :], mixes.at[at, :], in_sem.at[0, i]),
            pltpu.make_async_copy(layer_ref.at[at, :], layer.at[at, :], in_sem.at[1, i]),
            pltpu.make_async_copy(streams_ref.at[:, at, :], streams.at[:, at, :], in_sem.at[2, i]),
        )

    for i in range(MIX_TILES):
        for copy in incoming(i):
            copy.start()

    @pl.loop(0, MIX_TILES)
    def _(i):
        for copy in incoming(i):
            copy.wait()

        @pl.loop(0, tile // SUBLANES, unroll=4)
        def _(j):
            at = pl.ds(pl.multiple_of(i * tile + j * SUBLANES, SUBLANES), SUBLANES)
            layer_out = layer[at, :]
            weight = mixes[at, :]
            current = [streams[source, at, :] for source in range(STREAMS)]
            for target in range(STREAMS):
                value = weight[:, target : target + 1] * layer_out
                for source in range(STREAMS):
                    column = STREAMS * (1 + target) + source
                    value = value + weight[:, column : column + 1] * current[source]
                mixed[target, at, :] = value

        at = rows_of(i)
        pltpu.make_async_copy(mixed.at[:, at, :], out_ref.at[:, at, :], out_sem.at[0]).start()

    pltpu.make_async_copy(mixed, out_ref, out_sem.at[0]).wait()


def mix_streams(streams, layer_out, mixes):
    hbm = pl.BlockSpec(memory_space=pl.ANY)
    return pl.pallas_call(
        mix_kernel,
        in_specs=[hbm] * 3,
        out_specs=hbm,
        out_shape=jax.ShapeDtypeStruct(streams.shape, jnp.float32),
        scratch_shapes=[
            pltpu.VMEM(streams.shape, jnp.float32),
            pltpu.VMEM(layer_out.shape, jnp.float32),
            pltpu.VMEM(mixes.shape, jnp.float32),
            pltpu.VMEM(streams.shape, jnp.float32),
            pltpu.SemaphoreType.DMA((3, MIX_TILES)),
            pltpu.SemaphoreType.DMA((1,)),
        ],
        compiler_params=pltpu.CompilerParams(vmem_limit_bytes=67_043_328),
    )(streams, layer_out, mixes)


def solution(mesh):
    def body(streams, *rest):
        layer_out, mixes = feed_forward(mesh, streams, *rest)
        return mix_streams(streams, layer_out, mixes)

    placed = (
        P(None, "seq", "tensor"),
        P(None, None, "tensor"),
        P(),
        P(),
        P(),
        P("seq", "tensor"),
        P("seq", "tensor"),
        P("tensor", "seq"),
    )
    return jax.shard_map(body, mesh=mesh, in_specs=placed, out_specs=P(None, "seq", "tensor"), check_vma=False)
```

```python
import functools
import math

import jax
import jax.numpy as jnp
from jax import lax
from jax.experimental import pallas as pl
from jax.experimental.pallas import tpu as pltpu
from jax.sharding import PartitionSpec as P

STREAMS = 4
SWEEPS = 20
EPSILON = 0.25
LANES = 128
ROWS = 16
SPLITS = 2
MIX_TILES = 8
AHEAD = 2
MESH = pl.DeviceIdType.MESH
HIGHEST = lax.Precision.HIGHEST


def flip(index, offset):
    bit, out = 1, index
    while bit <= offset:
        if offset & bit:
            out = out + bit - 2 * bit * lax.rem(lax.div(index, bit), 2)
        bit *= 2
    return out


def last_bit(offset, order):
    if offset & 1:
        return 1
    return [b for b in order if offset & b][-1]


def width_of(size, limit):
    width = limit
    while size % width:
        width -= LANES
    return width


def plan_relays(n_seq, n_tensor, n_down, stages):
    hop, latency, unit, product = 5.6, 1.7, 9.8, 1.15
    last = len(stages) - 1
    middle = [o // 2 for r in range(1, last) for o in stages[r]]
    groups = []
    now = 0.0
    starts, ends = [], []

    def add(c, r, blocks_of, arrival):
        nonlocal now
        starts.append(max(now, arrival))
        now = starts[-1] + product * len(blocks_of)
        groups.append((c, r, blocks_of))
        ends.append(now)

    for c in range(n_down):
        add(c, 0, [0], 0.0)
    queue = [("own", c) for c in range(min(AHEAD, n_down))]
    for c in range(n_down):
        queue.append(("pass", c))
        if c + AHEAD < n_down:
            queue.append(("own", c + AHEAD))
    clock = 6.5 - unit
    for what, c in queue:
        clock += unit if what == "own" else unit / 2
        if what == "own":
            add(c, last - 1, middle, clock + 1.5)
        else:
            add(c, last, [stages[last][0] // 2], clock + 1.5)
    home = {(c, q): g for g, (c, _, blocks_of) in enumerate(groups) for q in blocks_of}
    final = len(groups) - 1

    def end(g):
        return ends[g] if g <= final else ends[final] + 2.0 * (g - final)

    def until(g):
        return starts[g + 1] - 1.0 if g < final else end(g)

    per = n_seq // n_tensor
    relayed, near = {}, {}
    for chip in range(n_seq // 2):
        for way in (1, -1):
            line = range(n_tensor) if way == 1 else range(n_tensor - 1, -1, -1)
            incoming = {}
            for place, z in enumerate(line):
                device = chip * n_tensor + z
                ahead = {step: (2 * (chip ^ step[1]) // per - z) * way for step in home}
                free_at, passed = 0.0, {}
                if place == 0:
                    held, sent = [], 0
                    for k in range(final + 1):
                        for step in [step for step, g in home.items() if g == k]:
                            if ahead[step] == 1:
                                held.append(step)
                            elif ahead[step] > 1:
                                free_at = max(free_at, ends[k]) + hop
                                passed[step] = (free_at + latency, k)
                        while held and (k == final or (sent < n_down - 1 and free_at < ends[k + 1])):
                            sent += 1
                            free_at = max(free_at, ends[k]) + hop
                            near.setdefault((k, held.pop(0)), []).append((free_at, device))
                else:
                    leaving = []
                    for step, g in home.items():
                        if ahead[step] <= 0:
                            continue
                        arrival, least = incoming[step]
                        k = max(g, least)
                        while max(until(k), end(k)) < arrival - 1.0:
                            k += 1
                        relayed.setdefault((k, step), []).append((arrival, device))
                        leaving.append((max(end(k), arrival), step, k))
                    for ready, step, k in sorted(leaving):
                        free_at = max(free_at, ready) + hop
                        passed[step] = (free_at + latency, k + 1)
                incoming = passed

    def by_group(found):
        plan = {}
        for (k, step), entries in sorted(found.items(), key=lambda item: min(item[1])[0]):
            plan.setdefault(k, []).append((step, sorted(d for _, d in entries)))
        return plan

    return groups, by_group(near), by_group(relayed)


def block_kernel(
    n_seq,
    n_tensor,
    bias_ref,
    scale_ref,
    mix_hbm,
    gain_ref,
    streams_ref,
    gate_ref,
    up_ref,
    down_ref,
    out_hbm,
    coef_hbm,
    base_hbm,
    mix_ref,
    out_ref,
    coef_ref,
    gate_buf,
    up_buf,
    down_buf,
    blocks,
    normed,
    hidden,
    arrived,
    tiles,
    base_parts,
    mix_parts,
    stats,
    columns,
    tile_sem,
    weight_send,
    weight_local,
    weight_recv,
    weight_pair,
    down_send,
    down_local,
    down_recv,
    down_pair,
    stat_send,
    stat_recv,
    input_send,
    input_recv,
    part_send,
    part_recv,
    edge_sem,
    base_sem,
    free,
):
    s, z = lax.axis_index("seq"), lax.axis_index("tensor")
    tokens, width = out_ref.shape
    features = width * n_tensor
    rows = features // n_seq
    n_gate, _, gate_width = gate_buf.shape
    n_down, pairs, units, block_width = down_buf.shape
    half = block_width // 2
    per = n_seq // n_tensor
    pair_blocks = per // 2
    own_blocks = n_down * pair_blocks
    piece = tiles.shape[2]
    tile = 2 * piece
    n_tiles = tokens // tile

    bits = []
    bit = 2
    while bit < n_seq:
        bits.append(bit)
        bit *= 2
    orders = (bits, bits[::-1])
    everything = n_seq - 2
    last = len(bits)

    def stage(o):
        return bin(o - o % 2).count("1")

    stages = [[o for o in range(0, n_seq, 2) if stage(o) == r] for r in range(last + 1)]

    def await_bytes(ref, sem):
        pltpu.make_async_copy(ref, ref, sem).wait()

    def peer(offset):
        return (flip(s, offset), z)

    def across(shift):
        return (s, lax.rem(z + shift, n_tensor))

    barrier = pltpu.get_barrier_semaphore()
    for b in [1] + bits:
        pl.semaphore_signal(barrier, inc=1, device_id=peer(b), device_id_type=MESH)
    for shift in range(1, n_tensor):
        pl.semaphore_signal(barrier, inc=1, device_id=across(shift), device_id_type=MESH)
    pl.semaphore_wait(barrier, len(bits) + n_tensor)

    weights = ((gate_ref, gate_buf), (up_ref, up_buf))

    def gate_slot(kind, c, o):
        return weights[kind][1].at[c, pl.ds(o * rows, rows), :]

    def gate_own(kind, c):
        return weights[kind][0].at[:, pl.ds(pl.multiple_of(c * gate_width, LANES), gate_width)]

    def gate_copy(kind, c, o):
        b = last_bit(o, orders[kind])
        source = gate_own(kind, c) if o == b else gate_slot(kind, c, o ^ b)
        return pltpu.make_async_remote_copy(
            src_ref=source,
            dst_ref=gate_slot(kind, c, o),
            send_sem=weight_send.at[kind],
            recv_sem=weight_pair.at[c] if o % 2 else weight_recv.at[c, stage(o) - 1],
            device_id=peer(b),
            device_id_type=MESH,
        )

    def gate_copy_local(kind, c):
        return pltpu.make_async_copy(gate_own(kind, c), gate_slot(kind, c, 0), weight_local.at[kind])

    def gate_arrival(c, r):
        await_bytes(gate_buf.at[c, pl.ds(0, 2 * len(stages[r]) * rows), :], weight_recv.at[c, r - 1])

    depth = units // 2

    def down_slot(kind, c, o):
        return down_buf.at[c, o // 2, pl.ds(kind * depth, depth), pl.ds((o % 2) * half, half)]

    def down_own(kind, c):
        return down_ref.at[pl.ds(kind * depth, depth), pl.ds(pl.multiple_of(c * half, LANES), half)]

    def down_copy(kind, c, o):
        b = last_bit(o, orders[kind])
        return pltpu.make_async_remote_copy(
            src_ref=down_own(kind, c) if o == b else down_slot(kind, c, o ^ b),
            dst_ref=down_slot(kind, c, o),
            send_sem=down_send.at[o % 2],
            recv_sem=down_pair.at[c, stage(o)] if o % 2 else down_recv.at[c, stage(o) - 1],
            device_id=peer(b),
            device_id_type=MESH,
        )

    def down_copy_local(kind, c):
        return pltpu.make_async_copy(down_own(kind, c), down_slot(kind, c, 0), down_local.at[c])

    def down_share(c, r):
        return down_buf.at[c, pl.ds(0, len(stages[r])), :, pl.ds(0, half)]

    def down_arrival(c, r):
        await_bytes(down_share(c, r), down_recv.at[c, r - 1])

    def down_pair_arrival(c, r):
        await_bytes(down_share(c, r), down_pair.at[c, r])

    def children(o, order):
        return [t for t in range(1, n_seq) if t ^ last_bit(t, order) == o and t != o]

    @pl.loop(0, n_gate)
    def _(c):
        for kind in (0, 1):
            for o in sorted(children(0, orders[kind]), key=lambda t: -t):
                gate_copy(kind, c, o).start()
            gate_copy_local(kind, c).start()

    mix_in = pltpu.make_async_copy(mix_hbm, mix_ref, edge_sem.at[0])
    coef_out = pltpu.make_async_copy(coef_ref, coef_hbm, edge_sem.at[1])
    mix_in.start()

    def tile_copy(i, slot):
        at = pl.ds(pl.multiple_of(i * tile + slot * piece, piece), piece)
        return pltpu.make_async_copy(streams_ref.at[:, at, :], tiles.at[slot], tile_sem.at[slot])

    def fetch(i, slot):
        @pl.when(i < n_tiles)
        def _():
            tile_copy(i, slot).start()

    for slot in (0, 1):
        tile_copy(0, slot).start()

    def halves(value):
        high = value.astype(jnp.bfloat16)
        return high, (value - high.astype(jnp.float32)).astype(jnp.bfloat16)

    n_logits = mix_ref.shape[0]
    mix_in.wait()
    for k in range(STREAMS):
        mix_parts[k] = jnp.concatenate(halves(mix_ref[:, k, :]))

    @pl.loop(0, n_tiles)
    def _(i):
        contract = (((1,), (1,)), ((), ()))
        found = []
        for slot in (0, 1):
            tile_copy(i, slot).wait()
            product = square = 0.0
            for k in range(STREAMS):
                current = tiles[slot, k]
                product += lax.dot_general(
                    mix_parts[k], jnp.concatenate(halves(current)), contract, preferred_element_type=jnp.float32
                )
                square += current * current
            product = product[:n_logits] + product[n_logits:]
            logits = product[:, :piece] + product[:, piece:]
            square = sum(square[:, j : j + LANES] for j in range(0, width, LANES))
            squares = lax.dot_general(
                jnp.ones((8, LANES), jnp.float32),
                square,
                contract,
                precision=HIGHEST,
                preferred_element_type=jnp.float32,
            )
            found.append(jnp.concatenate([logits, squares]))
            fetch(i + 1, slot)
        stats[0, :, pl.ds(pl.multiple_of(i * tile, LANES), tile)] = jnp.concatenate(found, axis=1)

    def stat_copy(shift):
        return pltpu.make_async_remote_copy(
            src_ref=stats.at[0],
            dst_ref=stats.at[shift],
            send_sem=stat_send.at[0],
            recv_sem=stat_recv.at[0],
            device_id=across(shift),
            device_id_type=MESH,
        )

    for shift in range(1, n_tensor):
        stat_copy(shift).start()
    for slot in (0, 1):
        tile_copy(0, slot).start()
    await_bytes(stats.at[pl.ds(1, n_tensor - 1)], stat_recv.at[0])
    total = stats[0]
    for shift in range(1, n_tensor):
        total = total + stats[shift]
    logits = total[:n_logits] * lax.rsqrt(total[n_logits : n_logits + 1] / (STREAMS * features) + EPSILON)

    def scaled(which, at):
        return scale_ref[which] * logits[at : at + 1] + bias_ref[at]

    pre = [jax.nn.sigmoid(scaled(0, k)) for k in range(STREAMS)]
    columns[...] = jnp.concatenate(pre + [jnp.zeros((LANES - STREAMS, tokens), jnp.float32)]).T

    def input_copy(way, hop, i, origin):
        at = (pl.ds(origin * own_blocks, own_blocks), pl.ds(pl.multiple_of(i * tile, tile), tile), slice(None))
        return pltpu.make_async_remote_copy(
            src_ref=blocks.at[at],
            dst_ref=blocks.at[at],
            send_sem=input_send.at[way, hop],
            recv_sem=input_recv.at[way, hop, i],
            device_id=(s, z + 1 - 2 * way),
            device_id_type=MESH,
        )

    def passes(way, hop):
        if way == 0:
            return jnp.logical_and(z >= hop, z + 1 < n_tensor)
        return jnp.logical_and(z + hop < n_tensor, z >= 1)

    def gets(way, hop):
        return z - 1 - hop >= 0 if way == 0 else z + 1 + hop < n_tensor

    def input_start(way, hop, i):
        @pl.when(passes(way, hop))
        def _():
            input_copy(way, hop, i, z - hop if way == 0 else z + hop).start()

    def input_wait(way, hop, i):
        @pl.when(gets(way, hop))
        def _():
            input_copy(way, hop, i, z - 1 - hop if way == 0 else z + 1 + hop).wait_recv()

    @pl.loop(0, n_tiles)
    def _(i):
        for slot in (0, 1):
            tile_copy(i, slot).wait()
            at = pl.ds(pl.multiple_of(i * tile + slot * piece, piece), piece)
            weight = columns[at, :]
            mixed = 0.0
            for k in range(STREAMS):
                mixed += weight[:, k : k + 1] * tiles[slot, k]
            mixed = mixed.astype(jnp.bfloat16)
            for j in range(own_blocks):
                blocks[z * own_blocks + j, at, :] = mixed[:, j * block_width : (j + 1) * block_width]
            fetch(i + 1, slot)
        for way in (0, 1):
            input_start(way, 0, i)

    for slot in (0, 1):
        tile_copy(0, slot).start()

    post = [2.0 * jax.nn.sigmoid(scaled(1, STREAMS + k)) for k in range(STREAMS)]
    start = tuple(jnp.exp(scaled(2, 2 * STREAMS + k)) for k in range(STREAMS * STREAMS))

    def balance(_, matrix):
        grid = [list(matrix[k * STREAMS : (k + 1) * STREAMS]) for k in range(STREAMS)]
        for k in range(STREAMS):
            row = grid[k][0] + grid[k][1] + grid[k][2] + grid[k][3]
            grid[k] = [g / row for g in grid[k]]
        for j in range(STREAMS):
            column = grid[0][j] + grid[1][j] + grid[2][j] + grid[3][j]
            for k in range(STREAMS):
                grid[k][j] = grid[k][j] / column
        return tuple(g for line in grid for g in line)

    res = lax.fori_loop(0, SWEEPS, balance, start)
    filler = LANES - STREAMS - STREAMS * STREAMS
    coef_ref[...] = jnp.concatenate(post + list(res) + [jnp.zeros((filler, tokens), jnp.float32)]).T

    coef_out.start()

    def base_copy(i, slot):
        at = pl.ds(pl.multiple_of(i * tile + slot * piece, piece), piece)
        return pltpu.make_async_copy(base_parts.at[slot], base_hbm.at[:, at, :], base_sem.at[slot])

    def mix_piece(hop, step):
        i, slot = hop * (n_tiles // 2) + lax.div(step, 2), lax.rem(step, 2)
        tile_copy(i, slot).wait()

        @pl.when(i > 0)
        def _():
            base_copy(i - 1, slot).wait()

        @pl.loop(0, piece // ROWS)
        def _(j):
            at = pl.ds(pl.multiple_of(j * ROWS, ROWS), ROWS)
            weight = coef_ref[pl.ds(pl.multiple_of(i * tile + slot * piece + j * ROWS, ROWS), ROWS), :]
            for part in range(2):
                lanes = pl.ds(part * (width // 2), width // 2)
                current = [tiles[slot, source, at, lanes] for source in range(STREAMS)]
                for target in range(STREAMS):
                    value = 0.0
                    for source in range(STREAMS):
                        column = STREAMS * (1 + target) + source
                        value += weight[:, column : column + 1] * current[source]
                    base_parts[slot, target, at, lanes] = value.astype(jnp.bfloat16)

        base_copy(i, slot).start()

        @pl.when(i + 1 < n_tiles)
        def _():
            tile_copy(i + 1, slot).start()

    for hop in range(max(n_tensor - 2, 2)):

        @pl.loop(0, n_tiles)
        def _(i):
            if hop < n_tensor - 2:
                for way in (0, 1):
                    input_wait(way, hop, i)
                    input_start(way, hop + 1, i)
            if hop < 2:
                mix_piece(hop, i)

    for slot in (0, 1):
        base_copy(n_tiles - 1, slot).wait()

    @pl.loop(0, n_gate)
    def _(c):
        for r in range(1, last):
            gate_arrival(c, r)
            for o in stages[r]:
                for kind in (0, 1):
                    for t in children(o, orders[kind]):
                        gate_copy(kind, c, t).start()

    def down_leave(c):
        for kind in (0, 1):
            for o in sorted(children(0, orders[kind]), key=lambda t: -t):
                if o != 1:
                    down_copy(kind, c, o).start()

    for c in range(n_down):
        for kind in (0, 1):
            down_copy(kind, c, 1).start()
            down_copy_local(kind, c).start()
    for c in range(min(AHEAD, n_down)):
        down_leave(c)

    granule = min(rows, block_width)

    @pl.loop(0, n_tiles)
    def _(i):
        at = pl.ds(pl.multiple_of(i * tile, tile), tile)
        for way in (0, 1):
            input_wait(way, n_tensor - 2, i)
        square = 0.0
        for j in range(n_tensor * own_blocks):
            value = blocks[j, at, :].astype(jnp.float32)
            square += value * value
        inverse = lax.rsqrt(jnp.sum(square, axis=1, keepdims=True) / features + EPSILON)
        for src in range(n_seq):
            o = flip(s, src)
            for g in range(rows // granule):
                col = src * rows + g * granule
                part = pl.ds(col % block_width, granule)
                value = blocks[col // block_width, at, part].astype(jnp.float32)
                value = value * inverse * gain_ref[pl.ds(col, granule)].astype(jnp.float32)[None, :]
                to = pl.ds(pl.multiple_of(o * rows + g * granule, LANES), granule)
                normed[at, to] = value.astype(jnp.bfloat16)

    for kind in (0, 1):
        await_bytes(weights[kind][1].at[:, pl.ds(0, rows), :], weight_local.at[kind])

    @pl.loop(0, n_gate)
    def _(c):
        gate_arrival(c, last)
        for kind in (0, 1):
            gate_copy(kind, c, everything + 1).start()
        await_bytes(gate_buf.at[c], weight_pair.at[c])
        gate_value = jnp.dot(normed[...], gate_buf[c], preferred_element_type=jnp.float32)
        up_value = jnp.dot(normed[...], up_buf[c], preferred_element_type=jnp.float32)
        to = pl.ds(pl.multiple_of(c * gate_width, LANES), gate_width)
        hidden[:, to] = (gate_value / (1.0 + jnp.exp(-gate_value)) * up_value).astype(jnp.bfloat16)

    def has(way):
        return z + 1 < n_tensor if way == 0 else z >= 1

    for way in (0, 1):

        @pl.when(has(way))
        def _():
            pl.semaphore_signal(free.at[way], inc=1, device_id=(s, z + 1 - 2 * way), device_id_type=MESH)

    for hop in range(n_tensor - 1):
        for way in (0, 1):

            @pl.when(passes(way, hop))
            def _():
                await_bytes(blocks.at[pl.ds(0, own_blocks)], input_send.at[way, hop])

    for way in (0, 1):

        @pl.when(has(way))
        def _():
            pl.semaphore_wait(free.at[1 - way], 1)

    stretch = tokens // SPLITS

    def place(c, q):
        source = flip(s, 2 * q)
        to = lax.div(source, per)
        at = c * pair_blocks + lax.rem(lax.div(source, 2), pair_blocks)
        return to, at, to * own_blocks + at

    def landing(from_right, at, index, part):
        at_rows = pl.ds(part * stretch, stretch)
        if from_right:
            return arrived.at[at, at_rows, :], part_recv.at[n_tensor * own_blocks + at, part]
        to = pl.ds(pl.multiple_of(index * block_width, LANES), block_width)
        return normed.at[at_rows, to], part_recv.at[index, part]

    def part_copy(c, q, part, way, from_right):
        _, at, index = place(c, q)
        target, arrival = landing(from_right, at, index, part)
        return pltpu.make_async_remote_copy(
            src_ref=blocks.at[index, pl.ds(part * stretch, stretch), :],
            dst_ref=target,
            send_sem=part_send.at[0],
            recv_sem=arrival,
            device_id=(s, z + 1 - 2 * way),
            device_id_type=MESH,
        )

    def part_start(c, q, part):
        to = place(c, q)[0]

        @pl.when(to > z)
        def _():
            part_copy(c, q, part, 0, False).start()

        @pl.when(to == z - 1)
        def _():
            part_copy(c, q, part, 1, True).start()

        @pl.when(to < z - 1)
        def _():
            part_copy(c, q, part, 1, False).start()

    def upstream(to):
        return jnp.where(to > z, z, jnp.where(to < z, n_tensor - 1 - z, 0))

    def project(c, q):
        value = jnp.dot(hidden[...], down_buf[c, q], preferred_element_type=jnp.float32).astype(jnp.bfloat16)
        to, _, index = place(c, q)
        core = lax.rem(s, 2)
        blocks[index, :, pl.ds(pl.multiple_of(core * half, LANES), half)] = value[:, :half]
        blocks[index, :, pl.ds(pl.multiple_of((1 - core) * half, LANES), half)] = value[:, half:]

        @pl.when(jnp.logical_and(upstream(to) == 0, jnp.abs(to - z) > 1))
        def _():
            for part in range(SPLITS):
                part_start(c, q, part)

    def relay(c, q):
        index = place(c, q)[2]

        @pl.loop(0, SPLITS)
        def _(part):
            part_copy(c, q, part, 0, False).wait_recv()

            @pl.loop(0, stretch // piece)
            def _(i):
                at = pl.ds(pl.multiple_of(part * stretch + i * piece, piece), piece)
                incoming = normed[at, pl.ds(pl.multiple_of(index * block_width, LANES), block_width)]
                value = blocks[index, at, :].astype(jnp.float32) + incoming.astype(jnp.float32)
                blocks[index, at, :] = value.astype(jnp.bfloat16)

            part_start(c, q, part)

    groups, near, due = plan_relays(n_seq, n_tensor, n_down, stages)
    device = lax.div(s, 2) * n_tensor + z

    def one_of(devices):
        return functools.reduce(jnp.logical_or, [device == d for d in devices])

    def send_near(group, steps):
        for (c, q), devices in near.get(group, []):
            if (c, q) in steps:

                @pl.when(one_of(devices))
                def _():
                    for part in range(SPLITS):
                        part_start(c, q, part)

    def relays(group):
        for (c, q), devices in due.get(group, []):

            @pl.when(one_of(devices))
            def _():
                relay(c, q)

    for group, (c, r, blocks_of) in enumerate(groups):
        if r > 0:
            first = range(1, last) if r < last else (last,)
            for level in first:
                down_arrival(c, level)
                for o in stages[level]:
                    for kind in (0, 1):
                        for t in children(o, orders[kind]):
                            down_copy(kind, c, t).start()
            if r < last and c + AHEAD < n_down:
                down_leave(c + AHEAD)
            for level in first:
                down_pair_arrival(c, level)
        else:
            await_bytes(down_buf.at[c, 0, :, pl.ds(0, half)], down_local.at[c])
            down_pair_arrival(c, 0)
        for q in blocks_of:
            project(c, q)
            send_near(group, [(c, q)])
        send_near(group, [step for step, _ in near.get(group, []) if step not in [(c, q) for q in blocks_of]])
        relays(group)
    for group in range(len(groups), max(due, default=-1) + 1):
        relays(group)

    for at in range(own_blocks):
        c, p = at // pair_blocks, at % pair_blocks
        index = z * own_blocks + at
        columns_of = [pl.ds((2 * p + h) * rows + c * half, half) for h in (0, 1)]
        for h in (0, 1):
            out_ref[:, columns_of[h]] = blocks[index, :, pl.ds(h * half, half)].astype(jnp.float32)
        for from_right in (False, True):

            @pl.when(has(0 if from_right else 1))
            def _():
                for part in range(SPLITS):
                    target, arrival = landing(from_right, at, index, part)
                    pltpu.make_async_remote_copy(
                        src_ref=blocks.at[index, pl.ds(part * stretch, stretch), :],
                        dst_ref=target,
                        send_sem=part_send.at[0],
                        recv_sem=arrival,
                        device_id=(s, z + 1 if from_right else z - 1),
                        device_id_type=MESH,
                    ).wait_recv()
                    at_rows = pl.ds(part * stretch, stretch)
                    for h in (0, 1):
                        if from_right:
                            value = arrived[at, at_rows, pl.ds(h * half, half)]
                        else:
                            to = pl.ds(pl.multiple_of(index * block_width + h * half, LANES), half)
                            value = normed[at_rows, to]
                        out_ref[at_rows, columns_of[h]] += value.astype(jnp.float32)

        for h in (0, 1):
            pltpu.make_async_copy(out_ref.at[:, columns_of[h]], out_hbm.at[:, columns_of[h]], edge_sem.at[2]).start()

    coef_out.wait()
    await_bytes(out_ref, edge_sem.at[2])
    await_bytes(stats.at[pl.ds(1, n_tensor - 1)], stat_send.at[0])
    for kind in (0, 1):
        await_bytes(weights[kind][1].at[:, pl.ds(rows, (n_seq - 1) * rows), :], weight_send.at[kind])
    await_bytes(down_buf.at[:, pl.ds(0, pairs - 1), :, pl.ds(0, half)], down_send.at[0])
    await_bytes(down_buf.at[:, :, :, pl.ds(0, half)], down_send.at[1])
    await_bytes(blocks.at[pl.ds(0, (n_tensor - 1) * own_blocks)], part_send.at[0])


def feed_forward(mesh, streams, mix_weight, mix_bias, mix_scale, norm_gain, gate_weight, up_weight, down_weight):
    n_seq, n_tensor = mesh.shape["seq"], mesh.shape["tensor"]
    tokens, width = streams.shape[1:]
    units = gate_weight.shape[1]
    rows = gate_weight.shape[0]
    features = width * n_tensor
    gate_width = width_of(units, 2 * LANES)
    n_gate = units // gate_width
    half = LANES
    n_down = down_weight.shape[1] // half
    own_blocks = width // (2 * half)
    tile = LANES
    n_tiles = tokens // tile
    exchanges = int(math.log2(n_seq)) - 1
    hbm, vmem = pl.BlockSpec(memory_space=pl.ANY), pl.BlockSpec(memory_space=pltpu.VMEM)
    smem = pl.BlockSpec(memory_space=pltpu.SMEM)
    dma = pltpu.SemaphoreType.DMA
    return pl.pallas_call(
        functools.partial(block_kernel, n_seq, n_tensor),
        out_shape=(
            jax.ShapeDtypeStruct((tokens, width), jnp.float32),
            jax.ShapeDtypeStruct((tokens, LANES), jnp.float32),
            jax.ShapeDtypeStruct(streams.shape, jnp.bfloat16),
        ),
        in_specs=[smem, smem, hbm, vmem, hbm, hbm, hbm, hbm],
        out_specs=(hbm, hbm, hbm),
        scratch_shapes=[
            pltpu.VMEM(mix_weight.shape, jnp.float32),
            pltpu.VMEM((tokens, width), jnp.float32),
            pltpu.VMEM((tokens, LANES), jnp.float32),
            pltpu.VMEM((n_gate, n_seq * rows, gate_width), jnp.bfloat16),
            pltpu.VMEM((n_gate, n_seq * rows, gate_width), jnp.bfloat16),
            pltpu.VMEM((n_down, n_seq // 2, units, 2 * half), jnp.bfloat16),
            pltpu.VMEM((n_tensor * own_blocks, tokens, 2 * half), jnp.bfloat16),
            pltpu.VMEM((tokens, features), jnp.bfloat16),
            pltpu.VMEM((tokens, units), jnp.bfloat16),
            pltpu.VMEM((own_blocks, tokens, 2 * half), jnp.bfloat16),
            pltpu.VMEM((2, STREAMS, tile // 2, width), jnp.float32),
            pltpu.VMEM((2, STREAMS, tile // 2, width), jnp.bfloat16),
            pltpu.VMEM((STREAMS, 2 * mix_weight.shape[0], width), jnp.bfloat16),
            pltpu.VMEM((n_tensor, mix_weight.shape[0] + 8, tokens), jnp.float32),
            pltpu.VMEM((tokens, LANES), jnp.float32),
            dma((2,)),
            dma((2,)),
            dma((2,)),
            dma((n_gate, exchanges)),
            dma((n_gate,)),
            dma((2,)),
            dma((n_down,)),
            dma((n_down, exchanges)),
            dma((n_down, exchanges + 1)),
            dma((1,)),
            dma((1,)),
            dma((2, n_tensor - 1)),
            dma((2, n_tensor - 1, n_tiles)),
            dma((1,)),
            dma(((n_tensor + 1) * own_blocks, SPLITS)),
            dma((3,)),
            dma((2,)),
            pltpu.SemaphoreType.REGULAR((2,)),
        ],
        compiler_params=pltpu.CompilerParams(
            collective_id=0, has_side_effects=True, vmem_limit_bytes=67_043_328
        ),
    )(mix_bias, mix_scale, mix_weight, norm_gain, streams, gate_weight, up_weight, down_weight)


def mix_kernel(base_ref, layer_ref, mix_ref, out_ref, base, layer, mixes, mixed, in_sem, out_sem):
    tile = layer.shape[0] // MIX_TILES

    def rows_of(i):
        return pl.ds(pl.multiple_of(i * tile, tile), tile)

    def incoming(i):
        at = rows_of(i)
        return (
            pltpu.make_async_copy(mix_ref.at[at, :], mixes.at[at, :], in_sem.at[0, i]),
            pltpu.make_async_copy(layer_ref.at[at, :], layer.at[at, :], in_sem.at[1, i]),
            pltpu.make_async_copy(base_ref.at[:, at, :], base.at[:, at, :], in_sem.at[2, i]),
        )

    for i in range(MIX_TILES):
        for copy in incoming(i):
            copy.start()

    @pl.loop(0, MIX_TILES)
    def _(i):
        for copy in incoming(i):
            copy.wait()

        @pl.loop(0, tile // ROWS, unroll=2)
        def _(j):
            at = pl.ds(pl.multiple_of(i * tile + j * ROWS, ROWS), ROWS)
            layer_out = layer[at, :]
            weight = mixes[at, :]
            for target in range(STREAMS):
                value = weight[:, target : target + 1] * layer_out
                mixed[target, at, :] = value + base[target, at, :].astype(jnp.float32)

        at = rows_of(i)
        pltpu.make_async_copy(mixed.at[:, at, :], out_ref.at[:, at, :], out_sem.at[0]).start()

    pltpu.make_async_copy(mixed, out_ref, out_sem.at[0]).wait()


def mix_streams(base, layer_out, mixes):
    hbm = pl.BlockSpec(memory_space=pl.ANY)
    return pl.pallas_call(
        mix_kernel,
        in_specs=[hbm] * 3,
        out_specs=hbm,
        out_shape=jax.ShapeDtypeStruct(base.shape, jnp.float32),
        scratch_shapes=[
            pltpu.VMEM(base.shape, base.dtype),
            pltpu.VMEM(layer_out.shape, jnp.float32),
            pltpu.VMEM(mixes.shape, jnp.float32),
            pltpu.VMEM(base.shape, jnp.float32),
            pltpu.SemaphoreType.DMA((3, MIX_TILES)),
            pltpu.SemaphoreType.DMA((1,)),
        ],
        compiler_params=pltpu.CompilerParams(vmem_limit_bytes=67_043_328),
    )(base, layer_out, mixes)


def solution(mesh):
    def body(streams, *rest):
        layer_out, mixes, base = feed_forward(mesh, streams, *rest)
        return mix_streams(base, layer_out, mixes)

    placed = (
        P(None, "seq", "tensor"),
        P(None, None, "tensor"),
        P(),
        P(),
        P(),
        P("seq", "tensor"),
        P("seq", "tensor"),
        P("tensor", "seq"),
    )
    return jax.shard_map(body, mesh=mesh, in_specs=placed, out_specs=P(None, "seq", "tensor"), check_vma=False)
```

```python
import functools
import math

import jax
import jax.numpy as jnp
from jax import lax
from jax.experimental import pallas as pl
from jax.experimental.pallas import tpu as pltpu
from jax.sharding import PartitionSpec as P

STREAMS = 4
SWEEPS = 20
EPSILON = 0.25
LANES = 128
ROWS = 16
SPLITS = 2
MIX_TILES = 8
AHEAD = 2
MESH = pl.DeviceIdType.MESH
HIGHEST = lax.Precision.HIGHEST


def flip(index, offset):
    bit, out = 1, index
    while bit <= offset:
        if offset & bit:
            out = out + bit - 2 * bit * lax.rem(lax.div(index, bit), 2)
        bit *= 2
    return out


def last_bit(offset, order):
    if offset & 1:
        return 1
    return [b for b in order if offset & b][-1]


def width_of(size, limit):
    width = limit
    while size % width:
        width -= LANES
    return width


def plan_relays(n_seq, n_tensor, n_down, stages):
    hop, latency, unit, product = 5.6, 1.7, 9.8, 1.15
    last = len(stages) - 1
    middle = [o // 2 for r in range(1, last) for o in stages[r]]
    groups = []
    now = 0.0
    starts, ends = [], []

    def add(c, r, blocks_of, arrival):
        nonlocal now
        starts.append(max(now, arrival))
        now = starts[-1] + product * len(blocks_of)
        groups.append((c, r, blocks_of))
        ends.append(now)

    for c in range(n_down):
        add(c, 0, [0], 0.0)
    queue = [("own", c) for c in range(min(AHEAD, n_down))]
    for c in range(n_down):
        queue.append(("pass", c))
        if c + AHEAD < n_down:
            queue.append(("own", c + AHEAD))
    clock = 6.5 - unit
    for what, c in queue:
        clock += unit if what == "own" else unit / 2
        if what == "own":
            add(c, last - 1, middle, clock + 1.5)
        else:
            add(c, last, [stages[last][0] // 2], clock + 1.5)
    home = {(c, q): g for g, (c, _, blocks_of) in enumerate(groups) for q in blocks_of}
    final = len(groups) - 1

    def end(g):
        return ends[g] if g <= final else ends[final] + 2.0 * (g - final)

    def until(g):
        return starts[g + 1] - 1.0 if g < final else end(g)

    per = n_seq // n_tensor
    relayed, near = {}, {}
    for chip in range(n_seq // 2):
        for way in (1, -1):
            line = range(n_tensor) if way == 1 else range(n_tensor - 1, -1, -1)
            incoming = {}
            for place, z in enumerate(line):
                device = chip * n_tensor + z
                ahead = {step: (2 * (chip ^ step[1]) // per - z) * way for step in home}
                free_at, passed = 0.0, {}
                if place == 0:
                    held, sent = [], 0
                    for k in range(final + 1):
                        for step in [step for step, g in home.items() if g == k]:
                            if ahead[step] == 1:
                                held.append(step)
                            elif ahead[step] > 1:
                                free_at = max(free_at, ends[k]) + hop
                                passed[step] = (free_at + latency, k)
                        while held and (k == final or (sent < n_down - 1 and free_at < ends[k + 1])):
                            sent += 1
                            free_at = max(free_at, ends[k]) + hop
                            near.setdefault((k, held.pop(0)), []).append((free_at, device))
                else:
                    leaving = []
                    for step, g in home.items():
                        if ahead[step] <= 0:
                            continue
                        arrival, least = incoming[step]
                        k = max(g, least)
                        while max(until(k), end(k)) < arrival - 1.0:
                            k += 1
                        relayed.setdefault((k, step), []).append((arrival, device))
                        leaving.append((max(end(k), arrival), step, k))
                    for ready, step, k in sorted(leaving):
                        free_at = max(free_at, ready) + hop
                        passed[step] = (free_at + latency, k + 1)
                incoming = passed

    def by_group(found):
        plan = {}
        for (k, step), entries in sorted(found.items(), key=lambda item: min(item[1])[0]):
            plan.setdefault(k, []).append((step, sorted(d for _, d in entries)))
        return plan

    return groups, by_group(near), by_group(relayed)


def block_kernel(
    n_seq,
    n_tensor,
    bias_ref,
    scale_ref,
    mix_hbm,
    gain_ref,
    streams_ref,
    gate_ref,
    up_ref,
    down_ref,
    out_hbm,
    coef_hbm,
    base_hbm,
    mix_ref,
    out_ref,
    out_stage,
    coef_ref,
    gate_buf,
    up_buf,
    down_buf,
    blocks,
    normed,
    hidden,
    arrived,
    tiles,
    base_parts,
    mix_parts,
    stats,
    columns,
    tile_sem,
    weight_send,
    weight_local,
    weight_recv,
    weight_pair,
    down_send,
    down_local,
    down_recv,
    down_pair,
    stat_send,
    stat_recv,
    input_send,
    input_recv,
    part_send,
    part_recv,
    edge_sem,
    base_sem,
    free,
):
    s, z = lax.axis_index("seq"), lax.axis_index("tensor")
    tokens, width = out_ref.shape
    features = width * n_tensor
    rows = features // n_seq
    n_gate, _, gate_width = gate_buf.shape
    n_down, pairs, units, block_width = down_buf.shape
    half = block_width // 2
    per = n_seq // n_tensor
    pair_blocks = per // 2
    own_blocks = n_down * pair_blocks
    piece = tiles.shape[2]
    tile = 2 * piece
    n_tiles = tokens // tile

    bits = []
    bit = 2
    while bit < n_seq:
        bits.append(bit)
        bit *= 2
    orders = (bits, bits[::-1])
    everything = n_seq - 2
    last = len(bits)

    def stage(o):
        return bin(o - o % 2).count("1")

    stages = [[o for o in range(0, n_seq, 2) if stage(o) == r] for r in range(last + 1)]

    def await_bytes(ref, sem):
        pltpu.make_async_copy(ref, ref, sem).wait()

    def peer(offset):
        return (flip(s, offset), z)

    def across(shift):
        return (s, lax.rem(z + shift, n_tensor))

    barrier = pltpu.get_barrier_semaphore()
    for b in [1] + bits:
        pl.semaphore_signal(barrier, inc=1, device_id=peer(b), device_id_type=MESH)
    for shift in range(1, n_tensor):
        pl.semaphore_signal(barrier, inc=1, device_id=across(shift), device_id_type=MESH)
    pl.semaphore_wait(barrier, len(bits) + n_tensor)

    weights = ((gate_ref, gate_buf), (up_ref, up_buf))

    def gate_slot(kind, c, o):
        return weights[kind][1].at[c, pl.ds(o * rows, rows), :]

    def gate_own(kind, c):
        return weights[kind][0].at[:, pl.ds(pl.multiple_of(c * gate_width, LANES), gate_width)]

    def gate_copy(kind, c, o):
        b = last_bit(o, orders[kind])
        source = gate_own(kind, c) if o == b else gate_slot(kind, c, o ^ b)
        return pltpu.make_async_remote_copy(
            src_ref=source,
            dst_ref=gate_slot(kind, c, o),
            send_sem=weight_send.at[kind],
            recv_sem=weight_pair.at[c] if o % 2 else weight_recv.at[c, stage(o) - 1],
            device_id=peer(b),
            device_id_type=MESH,
        )

    def gate_copy_local(kind, c):
        return pltpu.make_async_copy(gate_own(kind, c), gate_slot(kind, c, 0), weight_local.at[kind])

    def gate_arrival(c, r):
        await_bytes(gate_buf.at[c, pl.ds(0, 2 * len(stages[r]) * rows), :], weight_recv.at[c, r - 1])

    depth = units // 2

    def down_slot(kind, c, o):
        return down_buf.at[c, o // 2, pl.ds(kind * depth, depth), pl.ds((o % 2) * half, half)]

    def down_own(kind, c):
        return down_ref.at[pl.ds(kind * depth, depth), pl.ds(pl.multiple_of(c * half, LANES), half)]

    def down_copy(kind, c, o):
        b = last_bit(o, orders[kind])
        return pltpu.make_async_remote_copy(
            src_ref=down_own(kind, c) if o == b else down_slot(kind, c, o ^ b),
            dst_ref=down_slot(kind, c, o),
            send_sem=down_send.at[o % 2],
            recv_sem=down_pair.at[c, stage(o)] if o % 2 else down_recv.at[c, stage(o) - 1],
            device_id=peer(b),
            device_id_type=MESH,
        )

    def down_copy_local(kind, c):
        return pltpu.make_async_copy(down_own(kind, c), down_slot(kind, c, 0), down_local.at[c])

    def down_share(c, r):
        return down_buf.at[c, pl.ds(0, len(stages[r])), :, pl.ds(0, half)]

    def down_arrival(c, r):
        await_bytes(down_share(c, r), down_recv.at[c, r - 1])

    def down_pair_arrival(c, r):
        await_bytes(down_share(c, r), down_pair.at[c, r])

    def children(o, order):
        return [t for t in range(1, n_seq) if t ^ last_bit(t, order) == o and t != o]

    @pl.loop(0, n_gate)
    def _(c):
        for kind in (0, 1):
            for o in sorted(children(0, orders[kind]), key=lambda t: -t):
                gate_copy(kind, c, o).start()
            gate_copy_local(kind, c).start()

    mix_in = pltpu.make_async_copy(mix_hbm, mix_ref, edge_sem.at[0])
    coef_out = pltpu.make_async_copy(coef_ref, coef_hbm, edge_sem.at[1])
    mix_in.start()

    def tile_copy(i, slot):
        at = pl.ds(pl.multiple_of(i * tile + slot * piece, piece), piece)
        return pltpu.make_async_copy(streams_ref.at[:, at, :], tiles.at[slot], tile_sem.at[slot])

    def fetch(i, slot):
        @pl.when(i < n_tiles)
        def _():
            tile_copy(i, slot).start()

    for slot in (0, 1):
        tile_copy(0, slot).start()

    def halves(value):
        high = value.astype(jnp.bfloat16)
        return high, (value - high.astype(jnp.float32)).astype(jnp.bfloat16)

    n_logits = mix_ref.shape[0]
    mix_in.wait()
    for k in range(STREAMS):
        mix_parts[k] = jnp.concatenate(halves(mix_ref[:, k, :]))

    @pl.loop(0, n_tiles)
    def _(i):
        contract = (((1,), (1,)), ((), ()))
        found = []
        for slot in (0, 1):
            tile_copy(i, slot).wait()
            product = square = 0.0
            for k in range(STREAMS):
                current = tiles[slot, k]
                product += lax.dot_general(
                    mix_parts[k], jnp.concatenate(halves(current)), contract, preferred_element_type=jnp.float32
                )
                square += current * current
            product = product[:n_logits] + product[n_logits:]
            logits = product[:, :piece] + product[:, piece:]
            square = sum(square[:, j : j + LANES] for j in range(0, width, LANES))
            squares = lax.dot_general(
                jnp.ones((8, LANES), jnp.float32),
                square,
                contract,
                precision=HIGHEST,
                preferred_element_type=jnp.float32,
            )
            found.append(jnp.concatenate([logits, squares]))
            fetch(i + 1, slot)
        stats[0, :, pl.ds(pl.multiple_of(i * tile, LANES), tile)] = jnp.concatenate(found, axis=1)

    def stat_copy(shift):
        return pltpu.make_async_remote_copy(
            src_ref=stats.at[0],
            dst_ref=stats.at[shift],
            send_sem=stat_send.at[0],
            recv_sem=stat_recv.at[0],
            device_id=across(shift),
            device_id_type=MESH,
        )

    for shift in range(1, n_tensor):
        stat_copy(shift).start()
    for slot in (0, 1):
        tile_copy(0, slot).start()
    await_bytes(stats.at[pl.ds(1, n_tensor - 1)], stat_recv.at[0])
    total = stats[0]
    for shift in range(1, n_tensor):
        total = total + stats[shift]
    logits = total[:n_logits] * lax.rsqrt(total[n_logits : n_logits + 1] / (STREAMS * features) + EPSILON)

    def scaled(which, at):
        return scale_ref[which] * logits[at : at + 1] + bias_ref[at]

    pre = [jax.nn.sigmoid(scaled(0, k)) for k in range(STREAMS)]
    columns[...] = jnp.concatenate(pre + [jnp.zeros((LANES - STREAMS, tokens), jnp.float32)]).T

    def input_copy(way, hop, i, origin):
        at = (pl.ds(origin * own_blocks, own_blocks), pl.ds(pl.multiple_of(i * tile, tile), tile), slice(None))
        return pltpu.make_async_remote_copy(
            src_ref=blocks.at[at],
            dst_ref=blocks.at[at],
            send_sem=input_send.at[way, hop],
            recv_sem=input_recv.at[way, hop, i],
            device_id=(s, z + 1 - 2 * way),
            device_id_type=MESH,
        )

    def passes(way, hop):
        if way == 0:
            return jnp.logical_and(z >= hop, z + 1 < n_tensor)
        return jnp.logical_and(z + hop < n_tensor, z >= 1)

    def gets(way, hop):
        return z - 1 - hop >= 0 if way == 0 else z + 1 + hop < n_tensor

    def input_start(way, hop, i):
        @pl.when(passes(way, hop))
        def _():
            input_copy(way, hop, i, z - hop if way == 0 else z + hop).start()

    def input_wait(way, hop, i):
        @pl.when(gets(way, hop))
        def _():
            input_copy(way, hop, i, z - 1 - hop if way == 0 else z + 1 + hop).wait_recv()

    @pl.loop(0, n_tiles)
    def _(i):
        for slot in (0, 1):
            tile_copy(i, slot).wait()
            at = pl.ds(pl.multiple_of(i * tile + slot * piece, piece), piece)
            weight = columns[at, :]
            mixed = 0.0
            for k in range(STREAMS):
                mixed += weight[:, k : k + 1] * tiles[slot, k]
            mixed = mixed.astype(jnp.bfloat16)
            for j in range(own_blocks):
                blocks[z * own_blocks + j, at, :] = mixed[:, j * block_width : (j + 1) * block_width]
            fetch(i + 1, slot)
        for way in (0, 1):
            input_start(way, 0, i)

    for slot in (0, 1):
        tile_copy(0, slot).start()

    post = [2.0 * jax.nn.sigmoid(scaled(1, STREAMS + k)) for k in range(STREAMS)]
    start = tuple(jnp.exp(scaled(2, 2 * STREAMS + k)) for k in range(STREAMS * STREAMS))

    def balance(_, matrix):
        grid = [list(matrix[k * STREAMS : (k + 1) * STREAMS]) for k in range(STREAMS)]
        for k in range(STREAMS):
            row = grid[k][0] + grid[k][1] + grid[k][2] + grid[k][3]
            grid[k] = [g / row for g in grid[k]]
        for j in range(STREAMS):
            column = grid[0][j] + grid[1][j] + grid[2][j] + grid[3][j]
            for k in range(STREAMS):
                grid[k][j] = grid[k][j] / column
        return tuple(g for line in grid for g in line)

    res = lax.fori_loop(0, SWEEPS, balance, start)
    filler = LANES - STREAMS - STREAMS * STREAMS
    coef_ref[...] = jnp.concatenate(post + list(res) + [jnp.zeros((filler, tokens), jnp.float32)]).T

    coef_out.start()

    def base_copy(i, slot):
        at = pl.ds(pl.multiple_of(i * tile + slot * piece, piece), piece)
        return pltpu.make_async_copy(base_parts.at[slot], base_hbm.at[:, at, :], base_sem.at[slot])

    def mix_piece(hop, step):
        i, slot = hop * (n_tiles // 2) + lax.div(step, 2), lax.rem(step, 2)
        tile_copy(i, slot).wait()

        @pl.when(i > 0)
        def _():
            base_copy(i - 1, slot).wait()

        @pl.loop(0, piece // ROWS)
        def _(j):
            at = pl.ds(pl.multiple_of(j * ROWS, ROWS), ROWS)
            weight = coef_ref[pl.ds(pl.multiple_of(i * tile + slot * piece + j * ROWS, ROWS), ROWS), :]
            for part in range(2):
                lanes = pl.ds(part * (width // 2), width // 2)
                current = [tiles[slot, source, at, lanes] for source in range(STREAMS)]
                for target in range(STREAMS):
                    value = 0.0
                    for source in range(STREAMS):
                        column = STREAMS * (1 + target) + source
                        value += weight[:, column : column + 1] * current[source]
                    base_parts[slot, target, at, lanes] = value.astype(jnp.bfloat16)

        base_copy(i, slot).start()

        @pl.when(i + 1 < n_tiles)
        def _():
            tile_copy(i + 1, slot).start()

    for hop in range(max(n_tensor - 2, 2)):

        @pl.loop(0, n_tiles)
        def _(i):
            if hop < n_tensor - 2:
                for way in (0, 1):
                    input_wait(way, hop, i)
                    input_start(way, hop + 1, i)
            if hop < 2:
                mix_piece(hop, i)

    for slot in (0, 1):
        base_copy(n_tiles - 1, slot).wait()

    @pl.loop(0, n_gate)
    def _(c):
        for r in range(1, last):
            gate_arrival(c, r)
            for o in stages[r]:
                for kind in (0, 1):
                    for t in children(o, orders[kind]):
                        gate_copy(kind, c, t).start()

    def down_leave(c):
        for kind in (0, 1):
            for o in sorted(children(0, orders[kind]), key=lambda t: -t):
                if o != 1:
                    down_copy(kind, c, o).start()

    for c in range(n_down):
        for kind in (0, 1):
            down_copy(kind, c, 1).start()
            down_copy_local(kind, c).start()
    for c in range(min(AHEAD, n_down)):
        down_leave(c)

    granule = min(rows, block_width)

    @pl.loop(0, n_tiles)
    def _(i):
        at = pl.ds(pl.multiple_of(i * tile, tile), tile)
        for way in (0, 1):
            input_wait(way, n_tensor - 2, i)
        square = 0.0
        for j in range(n_tensor * own_blocks):
            value = blocks[j, at, :].astype(jnp.float32)
            square += value * value
        inverse = lax.rsqrt(jnp.sum(square, axis=1, keepdims=True) / features + EPSILON)
        for src in range(n_seq):
            o = flip(s, src)
            for g in range(rows // granule):
                col = src * rows + g * granule
                part = pl.ds(col % block_width, granule)
                value = blocks[col // block_width, at, part].astype(jnp.float32)
                value = value * inverse * gain_ref[pl.ds(col, granule)].astype(jnp.float32)[None, :]
                to = pl.ds(pl.multiple_of(o * rows + g * granule, LANES), granule)
                normed[at, to] = value.astype(jnp.bfloat16)

    for kind in (0, 1):
        await_bytes(weights[kind][1].at[:, pl.ds(0, rows), :], weight_local.at[kind])

    @pl.loop(0, n_gate)
    def _(c):
        gate_arrival(c, last)
        for kind in (0, 1):
            gate_copy(kind, c, everything + 1).start()
        await_bytes(gate_buf.at[c], weight_pair.at[c])
        gate_value = jnp.dot(normed[...], gate_buf[c], preferred_element_type=jnp.float32)
        up_value = jnp.dot(normed[...], up_buf[c], preferred_element_type=jnp.float32)
        to = pl.ds(pl.multiple_of(c * gate_width, LANES), gate_width)
        hidden[:, to] = (gate_value / (1.0 + jnp.exp(-gate_value)) * up_value).astype(jnp.bfloat16)

    def has(way):
        return z + 1 < n_tensor if way == 0 else z >= 1

    for way in (0, 1):

        @pl.when(has(way))
        def _():
            pl.semaphore_signal(free.at[way], inc=1, device_id=(s, z + 1 - 2 * way), device_id_type=MESH)

    for hop in range(n_tensor - 1):
        for way in (0, 1):

            @pl.when(passes(way, hop))
            def _():
                await_bytes(blocks.at[pl.ds(0, own_blocks)], input_send.at[way, hop])

    for way in (0, 1):

        @pl.when(has(way))
        def _():
            pl.semaphore_wait(free.at[1 - way], 1)

    stretch = tokens // SPLITS

    def place(c, q):
        source = flip(s, 2 * q)
        to = lax.div(source, per)
        at = c * pair_blocks + lax.rem(lax.div(source, 2), pair_blocks)
        return to, at, to * own_blocks + at

    def landing(from_right, at, index, part):
        at_rows = pl.ds(part * stretch, stretch)
        if from_right:
            return arrived.at[at, at_rows, :], part_recv.at[n_tensor * own_blocks + at, part]
        to = pl.ds(pl.multiple_of(index * block_width, LANES), block_width)
        return normed.at[at_rows, to], part_recv.at[index, part]

    def part_copy(c, q, part, way, from_right):
        _, at, index = place(c, q)
        target, arrival = landing(from_right, at, index, part)
        return pltpu.make_async_remote_copy(
            src_ref=blocks.at[index, pl.ds(part * stretch, stretch), :],
            dst_ref=target,
            send_sem=part_send.at[0],
            recv_sem=arrival,
            device_id=(s, z + 1 - 2 * way),
            device_id_type=MESH,
        )

    def part_start(c, q, part):
        to = place(c, q)[0]

        @pl.when(to > z)
        def _():
            part_copy(c, q, part, 0, False).start()

        @pl.when(to == z - 1)
        def _():
            part_copy(c, q, part, 1, True).start()

        @pl.when(to < z - 1)
        def _():
            part_copy(c, q, part, 1, False).start()

    def upstream(to):
        return jnp.where(to > z, z, jnp.where(to < z, n_tensor - 1 - z, 0))

    def project(c, q):
        value = jnp.dot(hidden[...], down_buf[c, q], preferred_element_type=jnp.float32).astype(jnp.bfloat16)
        to, _, index = place(c, q)
        core = lax.rem(s, 2)
        blocks[index, :, pl.ds(pl.multiple_of(core * half, LANES), half)] = value[:, :half]
        blocks[index, :, pl.ds(pl.multiple_of((1 - core) * half, LANES), half)] = value[:, half:]

        @pl.when(jnp.logical_and(upstream(to) == 0, jnp.abs(to - z) > 1))
        def _():
            for part in range(SPLITS):
                part_start(c, q, part)

    def relay(c, q):
        index = place(c, q)[2]

        @pl.loop(0, SPLITS)
        def _(part):
            part_copy(c, q, part, 0, False).wait_recv()

            @pl.loop(0, stretch // piece)
            def _(i):
                at = pl.ds(pl.multiple_of(part * stretch + i * piece, piece), piece)
                incoming = normed[at, pl.ds(pl.multiple_of(index * block_width, LANES), block_width)]
                value = blocks[index, at, :].astype(jnp.float32) + incoming.astype(jnp.float32)
                blocks[index, at, :] = value.astype(jnp.bfloat16)

            part_start(c, q, part)

    groups, near, due = plan_relays(n_seq, n_tensor, n_down, stages)
    device = lax.div(s, 2) * n_tensor + z

    def one_of(devices):
        return functools.reduce(jnp.logical_or, [device == d for d in devices])

    def send_near(group, steps):
        for (c, q), devices in near.get(group, []):
            if (c, q) in steps:

                @pl.when(one_of(devices))
                def _():
                    for part in range(SPLITS):
                        part_start(c, q, part)

    def relays(group):
        for (c, q), devices in due.get(group, []):

            @pl.when(one_of(devices))
            def _():
                relay(c, q)

    for group, (c, r, blocks_of) in enumerate(groups):
        if r > 0:
            first = range(1, last) if r < last else (last,)
            for level in first:
                down_arrival(c, level)
                for o in stages[level]:
                    for kind in (0, 1):
                        for t in children(o, orders[kind]):
                            down_copy(kind, c, t).start()
            if r < last and c + AHEAD < n_down:
                down_leave(c + AHEAD)
            for level in first:
                down_pair_arrival(c, level)
        else:
            await_bytes(down_buf.at[c, 0, :, pl.ds(0, half)], down_local.at[c])
            down_pair_arrival(c, 0)
        for q in blocks_of:
            project(c, q)
            send_near(group, [(c, q)])
        send_near(group, [step for step, _ in near.get(group, []) if step not in [(c, q) for q in blocks_of]])
        relays(group)
    for group in range(len(groups), max(due, default=-1) + 1):
        relays(group)

    for at in range(own_blocks):
        c, p = at // pair_blocks, at % pair_blocks
        index = z * own_blocks + at
        columns_of = [pl.ds((2 * p + h) * rows + c * half, half) for h in (0, 1)]
        for h in (0, 1):
            out_ref[:, columns_of[h]] = blocks[index, :, pl.ds(h * half, half)].astype(jnp.float32)
        for from_right in (False, True):

            @pl.when(has(0 if from_right else 1))
            def _():
                for part in range(SPLITS):
                    target, arrival = landing(from_right, at, index, part)
                    pltpu.make_async_remote_copy(
                        src_ref=blocks.at[index, pl.ds(part * stretch, stretch), :],
                        dst_ref=target,
                        send_sem=part_send.at[0],
                        recv_sem=arrival,
                        device_id=(s, z + 1 if from_right else z - 1),
                        device_id_type=MESH,
                    ).wait_recv()
                    at_rows = pl.ds(part * stretch, stretch)
                    for h in (0, 1):
                        if from_right:
                            value = arrived[at, at_rows, pl.ds(h * half, half)]
                        else:
                            to = pl.ds(pl.multiple_of(index * block_width + h * half, LANES), half)
                            value = normed[at_rows, to]
                        out_ref[at_rows, columns_of[h]] += value.astype(jnp.float32)

        for h in (0, 1):
            out_stage[:, columns_of[h]] = out_ref[:, columns_of[h]].astype(jnp.bfloat16)
            pltpu.make_async_copy(out_stage.at[:, columns_of[h]], out_hbm.at[:, columns_of[h]], edge_sem.at[2]).start()

    coef_out.wait()
    await_bytes(out_stage, edge_sem.at[2])
    await_bytes(stats.at[pl.ds(1, n_tensor - 1)], stat_send.at[0])
    for kind in (0, 1):
        await_bytes(weights[kind][1].at[:, pl.ds(rows, (n_seq - 1) * rows), :], weight_send.at[kind])
    await_bytes(down_buf.at[:, pl.ds(0, pairs - 1), :, pl.ds(0, half)], down_send.at[0])
    await_bytes(down_buf.at[:, :, :, pl.ds(0, half)], down_send.at[1])
    await_bytes(blocks.at[pl.ds(0, (n_tensor - 1) * own_blocks)], part_send.at[0])


def feed_forward(mesh, streams, mix_weight, mix_bias, mix_scale, norm_gain, gate_weight, up_weight, down_weight):
    n_seq, n_tensor = mesh.shape["seq"], mesh.shape["tensor"]
    tokens, width = streams.shape[1:]
    units = gate_weight.shape[1]
    rows = gate_weight.shape[0]
    features = width * n_tensor
    gate_width = width_of(units, 2 * LANES)
    n_gate = units // gate_width
    half = LANES
    n_down = down_weight.shape[1] // half
    own_blocks = width // (2 * half)
    tile = LANES
    n_tiles = tokens // tile
    exchanges = int(math.log2(n_seq)) - 1
    hbm, vmem = pl.BlockSpec(memory_space=pl.ANY), pl.BlockSpec(memory_space=pltpu.VMEM)
    smem = pl.BlockSpec(memory_space=pltpu.SMEM)
    dma = pltpu.SemaphoreType.DMA
    return pl.pallas_call(
        functools.partial(block_kernel, n_seq, n_tensor),
        out_shape=(
            jax.ShapeDtypeStruct((tokens, width), jnp.bfloat16),
            jax.ShapeDtypeStruct((tokens, LANES), jnp.float32),
            jax.ShapeDtypeStruct(streams.shape, jnp.bfloat16),
        ),
        in_specs=[smem, smem, hbm, vmem, hbm, hbm, hbm, hbm],
        out_specs=(hbm, hbm, hbm),
        scratch_shapes=[
            pltpu.VMEM(mix_weight.shape, jnp.float32),
            pltpu.VMEM((tokens, width), jnp.float32),
            pltpu.VMEM((tokens, width), jnp.bfloat16),
            pltpu.VMEM((tokens, LANES), jnp.float32),
            pltpu.VMEM((n_gate, n_seq * rows, gate_width), jnp.bfloat16),
            pltpu.VMEM((n_gate, n_seq * rows, gate_width), jnp.bfloat16),
            pltpu.VMEM((n_down, n_seq // 2, units, 2 * half), jnp.bfloat16),
            pltpu.VMEM((n_tensor * own_blocks, tokens, 2 * half), jnp.bfloat16),
            pltpu.VMEM((tokens, features), jnp.bfloat16),
            pltpu.VMEM((tokens, units), jnp.bfloat16),
            pltpu.VMEM((own_blocks, tokens, 2 * half), jnp.bfloat16),
            pltpu.VMEM((2, STREAMS, tile // 2, width), jnp.float32),
            pltpu.VMEM((2, STREAMS, tile // 2, width), jnp.bfloat16),
            pltpu.VMEM((STREAMS, 2 * mix_weight.shape[0], width), jnp.bfloat16),
            pltpu.VMEM((n_tensor, mix_weight.shape[0] + 8, tokens), jnp.float32),
            pltpu.VMEM((tokens, LANES), jnp.float32),
            dma((2,)),
            dma((2,)),
            dma((2,)),
            dma((n_gate, exchanges)),
            dma((n_gate,)),
            dma((2,)),
            dma((n_down,)),
            dma((n_down, exchanges)),
            dma((n_down, exchanges + 1)),
            dma((1,)),
            dma((1,)),
            dma((2, n_tensor - 1)),
            dma((2, n_tensor - 1, n_tiles)),
            dma((1,)),
            dma(((n_tensor + 1) * own_blocks, SPLITS)),
            dma((3,)),
            dma((2,)),
            pltpu.SemaphoreType.REGULAR((2,)),
        ],
        compiler_params=pltpu.CompilerParams(
            collective_id=0, has_side_effects=True, vmem_limit_bytes=67_043_328
        ),
    )(mix_bias, mix_scale, mix_weight, norm_gain, streams, gate_weight, up_weight, down_weight)


def mix_kernel(base_ref, layer_ref, mix_ref, out_ref, base, layer, mixes, mixed, in_sem, out_sem):
    tile = layer.shape[0] // MIX_TILES

    def rows_of(i):
        return pl.ds(pl.multiple_of(i * tile, tile), tile)

    def incoming(i):
        at = rows_of(i)
        return (
            pltpu.make_async_copy(mix_ref.at[at, :], mixes.at[at, :], in_sem.at[0, i]),
            pltpu.make_async_copy(layer_ref.at[at, :], layer.at[at, :], in_sem.at[1, i]),
            pltpu.make_async_copy(base_ref.at[:, at, :], base.at[:, at, :], in_sem.at[2, i]),
        )

    for i in range(MIX_TILES):
        for copy in incoming(i):
            copy.start()

    @pl.loop(0, MIX_TILES)
    def _(i):
        for copy in incoming(i):
            copy.wait()

        @pl.loop(0, tile // ROWS, unroll=2)
        def _(j):
            at = pl.ds(pl.multiple_of(i * tile + j * ROWS, ROWS), ROWS)
            layer_out = layer[at, :].astype(jnp.float32)
            weight = mixes[at, :]
            for target in range(STREAMS):
                value = weight[:, target : target + 1] * layer_out
                mixed[target, at, :] = value + base[target, at, :].astype(jnp.float32)

        at = rows_of(i)
        pltpu.make_async_copy(mixed.at[:, at, :], out_ref.at[:, at, :], out_sem.at[0]).start()

    pltpu.make_async_copy(mixed, out_ref, out_sem.at[0]).wait()


def mix_streams(base, layer_out, mixes):
    hbm = pl.BlockSpec(memory_space=pl.ANY)
    return pl.pallas_call(
        mix_kernel,
        in_specs=[hbm] * 3,
        out_specs=hbm,
        out_shape=jax.ShapeDtypeStruct(base.shape, jnp.float32),
        scratch_shapes=[
            pltpu.VMEM(base.shape, base.dtype),
            pltpu.VMEM(layer_out.shape, layer_out.dtype),
            pltpu.VMEM(mixes.shape, jnp.float32),
            pltpu.VMEM(base.shape, jnp.float32),
            pltpu.SemaphoreType.DMA((3, MIX_TILES)),
            pltpu.SemaphoreType.DMA((1,)),
        ],
        compiler_params=pltpu.CompilerParams(vmem_limit_bytes=67_043_328),
    )(base, layer_out, mixes)


def solution(mesh):
    def body(streams, *rest):
        layer_out, mixes, base = feed_forward(mesh, streams, *rest)
        return mix_streams(base, layer_out, mixes)

    placed = (
        P(None, "seq", "tensor"),
        P(None, None, "tensor"),
        P(),
        P(),
        P(),
        P("seq", "tensor"),
        P("seq", "tensor"),
        P("tensor", "seq"),
    )
    return jax.shard_map(body, mesh=mesh, in_specs=placed, out_specs=P(None, "seq", "tensor"), check_vma=False)
```
